256 devices in a mesh: img: 16 (over x, z_lo, core), patch: 16 (over y, z_hi).
Axes of the slice: x: 4, y: 4, z: 8 (z_hi: 4, z_lo: 2; z = z_hi * 2 + z_lo), core: 2. Of those that a mesh axis runs over, the one named last changes fastest.
Arguments:
- hidden: bfloat16 [32, 16, 128, 640], P('img', 'patch'), may hold values from -100 to 100
- stale_attn_in: bfloat16 [32, 16, 128, 640], P('img', 'patch'), may hold values from -100 to 100
- stale_conv_in: bfloat16 [32, 16, 128, 640], P('img', 'patch'), may hold values from -6 to 6
- ln_gain: float32 [640], replicated, may hold values from 0.25 to 1.75
- ln_bias: float32 [640], replicated, may hold values from -2 to 2
- w_qkv: bfloat16 [640, 1920], replicated, may hold values from -3 to 3
- w_out: bfloat16 [640, 640], replicated, may hold values from -0.25 to 0.25
- gn_gain: float32 [640], replicated, may hold values from 0.25 to 1.75
- gn_bias: float32 [640], replicated, may hold values from -1.5 to 1.5
- conv_weight: bfloat16 [3, 3, 640, 640], replicated, may hold values from -0.078125 to 0.078125
- conv_bias: float32 [640], replicated, may hold values from -1.5 to 1.5
- time_shift: float32 [32, 640], P('img'), may hold values from -6 to 6
Outputs:
- block_out: bfloat16 [32, 16, 128, 640], P('img', 'patch')
The draws below stay inside these ranges and needn't reach their ends.
All inputs are finite; a program needn't handle non-finite values.
Results may differ from the reference program's by a relative error of at most 0.0075.
The reference program's roundings to bfloat16 on the way count: a program that leaves them out, or rounds other values in their place, can miss the bound.
Values may be sent and summed in bfloat16 or wider, within the bound.
A program may use at most 128 MiB of HBM per device.

```python
import math
import jax
import jax.numpy as jnp
from jax import lax

C = 640
GROUPS = 32
HEAD_DIM = 64
ROWS_DEV = 1
COLS = 128
SAMPLES = 32
ROWS = 16
N_PATCH = 16


def paired_inputs(key):
    base_key = jax.random.fold_in(key, 101)
    subkeys = jax.random.split(base_key, 7)
    full_shape = (SAMPLES, ROWS, COLS, C)
    noise_current = jax.random.truncated_normal(subkeys[0], -4.0, 4.0, full_shape, jnp.float32)
    noise_stale = jax.random.truncated_normal(subkeys[1], -4.0, 4.0, full_shape, jnp.float32)
    pattern = 1.5 * jax.random.truncated_normal(subkeys[6], -4.0, 4.0, (SAMPLES, ROWS, 1, C), jnp.float32)
    row_frac = (jnp.arange(ROWS, dtype=jnp.float32) + 0.5) / ROWS - 0.5
    row_scale = 10.0 ** (row_frac[None, :] + 0.5 * jax.random.uniform(subkeys[2], (SAMPLES, ROWS), jnp.float32) - 0.25)
    col_scale = 2.0 ** (2.0 * jax.random.uniform(subkeys[3], (SAMPLES, COLS), jnp.float32) - 1.0)
    chan_scale = 2.0 ** (2.0 * jax.random.uniform(subkeys[4], (C,), jnp.float32) - 1.0)
    full_scale = row_scale[:, :, None, None] * col_scale[:, None, :, None] * chan_scale
    current = (noise_current + pattern) * full_scale
    stale = (noise_stale + pattern) * full_scale
    current = jnp.clip(current, -96.0, 96.0) * 0.03
    stale = jnp.clip(stale, -96.0, 96.0)
    return (current, stale)


def draw_hidden(key, part):
    return paired_inputs(key)[0].astype(jnp.bfloat16)


def draw_stale_attn_in(key, part):
    return paired_inputs(key)[1].astype(jnp.bfloat16)


def draw_ln_bias(key, part):
    bias_scale = 0.3
    return bias_scale * jax.random.truncated_normal(jax.random.fold_in(key, 303), -4.0, 4.0, (C,), jnp.float32)


def draw_w_qkv(key, part):
    subkeys = jax.random.split(jax.random.fold_in(key, 202), 4)
    query_cols = jax.random.truncated_normal(subkeys[0], -4.0, 4.0, (C, C), jnp.float32) / math.sqrt(C)
    value_cols = jax.random.truncated_normal(subkeys[1], -4.0, 4.0, (C, C), jnp.float32) / math.sqrt(C)
    query_cols = 2.5 * query_cols
    key_cols = jax.random.truncated_normal(subkeys[3], -4.0, 4.0, (C, C), jnp.float32) / math.sqrt(C)
    return jnp.concatenate([query_cols, key_cols, value_cols], 1).astype(jnp.bfloat16)


def block_scale(own_key, extent, pieces, smallest, high):
    factor_of, own = 1.0, jax.random.fold_in(own_key, 6)
    for axis_at, blocks in pieces:
        steps = jnp.exp(jax.random.uniform(jax.random.fold_in(own, axis_at), (blocks,), jnp.float32, smallest / len(pieces), high / len(pieces)))
        factor_of = factor_of * jnp.repeat(steps, extent[axis_at] // blocks).reshape([-1 if axis == axis_at else 1 for axis in range(len(extent))])
    return factor_of


def noise(own_key, shape, scale, reach, cuts=(), kind=jnp.bfloat16):
    drawn = jax.random.normal(own_key, shape, jnp.float32) * scale
    if len(cuts) > 0:
        drawn = block_scale(own_key, shape, cuts, -0.22, 0.18) * drawn
    return jnp.clip(drawn, min=-reach, max=reach).astype(kind)


def setup_inputs(seed: int = 0) -> dict:
    seeds = jax.random.split(jax.random.key(seed), 13)
    return {
        "hidden": draw_hidden(jax.random.fold_in(seeds[12], 71), 0),
        "stale_attn_in": draw_stale_attn_in(jax.random.fold_in(seeds[12], 71), 0),
        "stale_conv_in": noise(seeds[2], (SAMPLES, ROWS, COLS, C), 1.0, 6.0, ((0, 16), (1, 16))),
        "ln_gain": jnp.clip(1.0 + 0.15 * jax.random.normal(seeds[3], (C,), jnp.float32), 0.25, 1.75),
        "ln_bias": draw_ln_bias(jax.random.fold_in(seeds[12], 71), 0),
        "w_qkv": draw_w_qkv(jax.random.fold_in(seeds[12], 71), 0),
        "w_out": noise(seeds[6], (C, C), C ** -0.5, 0.25),
        "gn_gain": jnp.clip(1.0 + 0.15 * jax.random.normal(seeds[7], (C,), jnp.float32), 0.25, 1.75),
        "gn_bias": noise(seeds[8], (C,), 0.3, 1.5, (), jnp.float32),
        "conv_weight": noise(seeds[9], (3, 3, C, C), (9 * C) ** -0.5, 0.078125),
        "conv_bias": noise(seeds[10], (C,), 0.3, 1.5, (), jnp.float32),
        "time_shift": noise(seeds[11], (SAMPLES, C), 1.0, 6.0, ((0, 16),), jnp.float32),
    }


EPSILON = 1e-05

def to_half(values):
    return lax.optimization_barrier(values.astype(jnp.bfloat16))

def layer_norm(values, gain, bias):
    values = values.astype(jnp.float32)
    centre = lax.optimization_barrier(jnp.mean(values, -1, keepdims=True))
    centred = values - centre
    spread = lax.optimization_barrier(jnp.mean(centred * centred, -1, keepdims=True))
    return to_half(centred * lax.rsqrt(spread + EPSILON) * gain + bias)

def reference(hidden, stale_attn_in, stale_conv_in, ln_gain, ln_bias, w_qkv, w_out, gn_gain, gn_bias, conv_weight, conv_bias, time_shift):
    head_count = C // HEAD_DIM
    tokens = ROWS * COLS
    patches = N_PATCH
    per_patch = ROWS_DEV * COLS
    score_scale = HEAD_DIM ** (-0.5)
    fresh_in = layer_norm(hidden, ln_gain, ln_bias).reshape(SAMPLES, tokens, C)
    stale_in = layer_norm(stale_attn_in, ln_gain, ln_bias).reshape(SAMPLES, tokens, C)

    def split_heads(values):
        return values.reshape(patches, per_patch, head_count, HEAD_DIM).transpose(2, 0, 1, 3)

    def one_head(head_parts):
        queries, fresh_keys, fresh_values, stale_keys, stale_values = head_parts
        queries = queries.astype(jnp.float32)
        remote = jnp.einsum('pqd,rkd->pqrk', queries, stale_keys.astype(jnp.float32)) * score_scale
        local_scores = jnp.einsum('pqd,pkd->pqk', queries, fresh_keys.astype(jnp.float32)) * score_scale
        same_patch = jnp.eye(patches, dtype=bool)[:, None, :, None]
        remote = jnp.where(same_patch, -jnp.inf, remote)
        row_max = jnp.maximum(lax.optimization_barrier(jnp.max(remote, axis=(2, 3))), lax.optimization_barrier(jnp.max(local_scores, -1)))
        remote_weights = jnp.exp(remote - row_max[:, :, None, None])
        local_weights = jnp.exp(local_scores - row_max[:, :, None])
        weight_sum = lax.optimization_barrier(jnp.sum(remote_weights, axis=(2, 3))) + lax.optimization_barrier(jnp.sum(local_weights, -1))
        gathered = jnp.einsum('pqrk,rkd->pqd', to_half(remote_weights).astype(jnp.float32), stale_values.astype(jnp.float32))
        gathered = gathered + jnp.einsum('pqk,pkd->pqd', to_half(local_weights).astype(jnp.float32), fresh_values.astype(jnp.float32))
        return gathered / weight_sum[:, :, None]

    def attend_sample(operands):
        fresh_rows, stale_rows = operands
        projected = to_half(jnp.dot(fresh_rows, w_qkv, preferred_element_type=jnp.float32))
        stale_pairs = to_half(jnp.dot(stale_rows, w_qkv[:, C:], preferred_element_type=jnp.float32))
        head_parts = (split_heads(projected[:, :C]), split_heads(projected[:, C:2 * C]), split_heads(projected[:, 2 * C:]), split_heads(stale_pairs[:, :C]), split_heads(stale_pairs[:, C:]))
        per_head = lax.map(one_head, head_parts)
        attended = to_half(per_head.transpose(1, 2, 0, 3).reshape(tokens, C))
        return jnp.dot(attended, w_out, preferred_element_type=jnp.float32)
    attention_out = lax.map(attend_sample, (fresh_in, stale_in))
    residual = to_half(hidden.reshape(SAMPLES, tokens, C).astype(jnp.float32) + attention_out)
    grouped = residual.astype(jnp.float32).reshape(SAMPLES, tokens, GROUPS, C // GROUPS)
    group_mean = lax.optimization_barrier(jnp.mean(grouped, axis=(1, 3), keepdims=True))
    centred = grouped - group_mean
    group_var = lax.optimization_barrier(jnp.mean(centred * centred, axis=(1, 3), keepdims=True))
    normalized = (centred * lax.rsqrt(group_var + EPSILON)).reshape(SAMPLES, tokens, C)
    activated = to_half(jax.nn.silu(normalized * gn_gain + gn_bias)).reshape(SAMPLES, ROWS, COLS, C)

    def convolve(operands):
        fresh_rows, stale_rows = operands
        fresh_patch = fresh_rows.reshape(patches, ROWS_DEV, COLS, C)
        stale_patch = stale_rows.reshape(patches, ROWS_DEV, COLS, C)
        zero_rim = jnp.zeros((1, 1, COLS, C), jnp.bfloat16)
        rim_above = jnp.concatenate([zero_rim, stale_patch[:-1, ROWS_DEV - 1:]], 0)
        rim_below = jnp.concatenate([stale_patch[1:, :1], zero_rim], 0)
        framed = jnp.concatenate([rim_above, fresh_patch, rim_below], 1)
        framed = jnp.pad(framed, ((0, 0), (0, 0), (1, 1), (0, 0)))
        summed = jnp.zeros((patches * ROWS_DEV * COLS, C), jnp.float32)
        for tap_row in range(3):
            for tap_col in range(3):
                window = framed[:, tap_row:tap_row + ROWS_DEV, tap_col:tap_col + COLS, :].reshape(-1, C)
                summed = summed + jnp.dot(window, conv_weight[tap_row, tap_col], preferred_element_type=jnp.float32)
        return summed.reshape(ROWS, COLS, C)
    convolved = lax.map(convolve, (activated, stale_conv_in))
    summed_out = convolved + conv_bias + time_shift[:, None, None, :] + residual.astype(jnp.float32).reshape(SAMPLES, ROWS, COLS, C)
    return summed_out.astype(jnp.bfloat16)
```

```python
import functools

import jax
import jax.numpy as jnp
from jax import lax
from jax.experimental import pallas as pl
from jax.experimental.pallas import tpu as pltpu
from jax.sharding import PartitionSpec as P

GROUPS = 32
HEAD_DIM = 64
SIDE = 4
EPSILON = 1e-05
MESH = pl.DeviceIdType.MESH
F32 = jnp.float32
BF16 = jnp.bfloat16


def dot_nt(a, b):
    return lax.dot_general(a, b, (((1,), (1,)), ((), ())), preferred_element_type=F32)


def dot(a, b):
    return jnp.dot(a, b, preferred_element_type=F32)


def kernel(
    hidden_hbm,
    stale_hbm,
    rim_hbm,
    ln_gain_hbm,
    ln_bias_hbm,
    w_qkv_hbm,
    w_out_hbm,
    gn_gain_hbm,
    gn_bias_hbm,
    conv_w_hbm,
    conv_b_hbm,
    shift_hbm,
    out_ref,
    hidden,
    stale,
    rim_own,
    rim_near,
    ln_gain,
    ln_bias,
    w_qkv,
    w_out,
    gn_gain,
    gn_bias,
    conv_w,
    conv_b,
    shift,
    fresh,
    zbuf,
    qbuf,
    kv,
    part,
    part_in,
    lse,
    lse_in,
    att,
    res,
    gst,
    proj,
    rim_sum,
    act,
    load_sem,
    zsend,
    zrecv,
    qsend,
    qrecv,
    osend,
    orecv,
    rsend,
    rrecv,
    gsend,
    grecv,
):
    n_patch = SIDE * SIDE
    samples, tokens, chans = hidden.shape
    half = tokens // 2
    p = lax.axis_index("patch")
    y, z = p // SIDE, p % SIDE
    z_next = {"patch": y * SIDE + (z + 1) % SIDE}
    z_prev = {"patch": y * SIDE + (z + SIDE - 1) % SIDE}
    y_next = {"patch": ((y + 1) % SIDE) * SIDE + z}
    y_prev = {"patch": ((y + SIDE - 1) % SIDE) * SIDE + z}
    y_far = {"patch": ((y + 2) % SIDE) * SIDE + z}

    def peer(k):
        return {"patch": (p + k) % n_patch}

    loads = []
    for i, (src, dst) in enumerate(
        (
            (stale_hbm, stale),
            (ln_gain_hbm, ln_gain),
            (ln_bias_hbm, ln_bias),
            (hidden_hbm, hidden),
            (w_qkv_hbm, w_qkv),
            (rim_hbm, rim_own),
            (w_out_hbm, w_out),
            (gn_gain_hbm, gn_gain),
            (gn_bias_hbm, gn_bias),
            (conv_b_hbm, conv_b),
            (shift_hbm, shift),
            (conv_w_hbm, conv_w),
        )
    ):
        load = pltpu.make_async_copy(src, dst, load_sem.at[i])
        load.start()
        loads.append(load)

    barrier = pltpu.get_barrier_semaphore()
    for k in range(1, n_patch):
        pl.semaphore_signal(barrier, inc=1, device_id=peer(k), device_id_type=MESH)

    def remote(src, dst, send, recv, target):
        return pltpu.make_async_remote_copy(
            src_ref=src, dst_ref=dst, send_sem=send, recv_sem=recv, device_id=target, device_id_type=MESH
        )

    def ring(buf, send, recv, s, nxt, prv):
        return (
            remote(buf.at[s, 0], buf.at[s, 1], send.at[s, 0], recv.at[s, 0], nxt),
            remote(buf.at[s, 0], buf.at[s, 2], send.at[s, 1], recv.at[s, 1], prv),
            remote(
                buf.at[s, 1, pl.ds(0, half)], buf.at[s, 3, pl.ds(0, half)], send.at[s, 2], recv.at[s, 2], nxt
            ),
            remote(
                buf.at[s, 2, pl.ds(half, half)],
                buf.at[s, 3, pl.ds(half, half)],
                send.at[s, 3],
                recv.at[s, 3],
                prv,
            ),
        )

    zc = [ring(zbuf, zsend, zrecv, s, z_next, z_prev) for s in range(samples)]
    qc = [ring(qbuf, qsend, qrecv, s, y_next, y_prev) for s in range(samples)]

    def layer_norm(values):
        values = values.astype(F32)
        centre = jnp.mean(values, -1, keepdims=True)
        centred = values - centre
        spread = jnp.mean(centred * centred, -1, keepdims=True)
        return (centred * lax.rsqrt(spread + EPSILON) * ln_gain[...] + ln_bias[...]).astype(BF16)

    step = 32
    for load in loads[:3]:
        load.wait()
    for s in range(samples):

        @pl.loop(0, tokens // step)
        def _(i):
            rows = pl.ds(pl.multiple_of(i * step, step), step)
            zbuf[s, 0, rows] = layer_norm(stale[s, rows])

    loads[3].wait()
    for s in range(samples):

        @pl.loop(0, tokens // step)
        def _(i):
            rows = pl.ds(pl.multiple_of(i * step, step), step)
            fresh[s, rows] = layer_norm(hidden[s, rows])

    pl.semaphore_wait(barrier, n_patch - 1)
    for s in range(samples):
        zc[s][0].start()
        zc[s][1].start()

    loads[4].wait()
    for s in range(samples):
        for c in range(0, chans, 128):
            q = dot(fresh[s], w_qkv[:, c : c + 128]).astype(BF16)
            qbuf[s, 0, :, c : c + 128] = q * BF16(HEAD_DIM**-0.5)
        qc[s][0].start()
        qc[s][1].start()

    def project(src, s, block):
        for c in range(0, 2 * chans, 256):
            kv[s, block * tokens : (block + 1) * tokens, c : c + 256] = dot(
                src, w_qkv[:, chans + c : chans + c + 256]
            ).astype(BF16)

    for s in range(samples):
        project(fresh[s], s, 0)
        project(zbuf[s, 0], s, 4)

    width = chans // GROUPS

    def group_of(v):
        return (v * (65536 // width + 1)) >> 16

    for r in range(0, chans, 128):
        same = group_of(lax.broadcasted_iota(jnp.int32, (128, chans), 0) + r) == group_of(
            lax.broadcasted_iota(jnp.int32, (128, chans), 1)
        )
        proj[r : r + 128] = jnp.where(same, 1.0, 0.0).astype(BF16)

    for s in range(samples):
        qc[s][0].wait_recv()
        qc[s][2].start()
        qc[s][1].wait_recv()
        qc[s][3].start()
        zc[s][0].wait_recv()
        zc[s][2].start()
        zc[s][1].wait_recv()
        zc[s][3].start()
        project(zbuf[s, 1], s, 1)
        project(zbuf[s, 2], s, 2)

    loads[5].wait()
    down = remote(rim_own, rim_near.at[0], rsend.at[0], rrecv.at[0], peer(1))
    up = remote(rim_own, rim_near.at[1], rsend.at[1], rrecv.at[1], peer(n_patch - 1))

    @pl.when(p < n_patch - 1)
    def _():
        down.start()

    @pl.when(p > 0)
    def _():
        up.start()

    @pl.when(p == 0)
    def _():
        rim_near[0] = jnp.zeros(rim_near.shape[1:], BF16)

    @pl.when(p == n_patch - 1)
    def _():
        rim_near[1] = jnp.zeros(rim_near.shape[1:], BF16)

    lane = lax.broadcasted_iota(jnp.int32, (tokens, 128), 1)
    low = lane < HEAD_DIM
    keys = SIDE * tokens
    pairs = chans // 128

    def attend(s):
        lse[s] = jnp.zeros(lse.shape[1:], F32)

        @pl.loop(0, pairs)
        def _(j):
            cols = pl.ds(pl.multiple_of(j * 128, 128), 128)
            vcols = pl.ds(pl.multiple_of(chans + j * 128, 128), 128)
            for b in range(SIDE):
                rows = pl.ds(0 if b == 0 else tokens, keys)
                kp = kv[s, rows, cols]
                vp = kv[s, rows, vcols]
                qp = qbuf[s, b, :, cols]
                klow = lax.broadcasted_iota(jnp.int32, (keys, 128), 1) < HEAD_DIM
                outs, tops = [], []
                for h in range(2):
                    mine = low if h == 0 else ~low
                    kmine = klow if h == 0 else ~klow
                    scores = dot_nt(jnp.where(mine, qp, BF16(0)), kp)
                    top = jnp.max(scores, -1, keepdims=True)
                    w = jnp.exp(scores - top).astype(BF16)
                    outs.append(dot(w, jnp.where(kmine, vp, BF16(1))))
                    tops.append(top)
                total = pltpu.roll(jnp.where(low, outs[1], outs[0]), HEAD_DIM, 1)
                part[s, b, :, cols] = (jnp.where(low, outs[0], outs[1]) / total).astype(BF16)
                level = jnp.where(low, tops[0], tops[1]) + jnp.log(total)
                lse[s, b] = jnp.where((lane & (HEAD_DIM - 1)) == j, level, lse[s, b])

    oc = []
    for s in range(samples):
        copies = []
        for i, (b, there, target) in enumerate(((1, 2, y_prev), (2, 1, y_next), (3, 3, y_far))):
            copies.append(
                remote(part.at[s, b], part_in.at[s, there], osend.at[s, i, 0], orecv.at[s, there - 1, 0], target)
            )
            copies.append(
                remote(
                    lse_in.at[s, b, 0], lse_in.at[s, there, 1], osend.at[s, i, 1], orecv.at[s, there - 1, 1], target
                )
            )
        oc.append(copies)

    for s in range(samples):
        qc[s][2].wait_recv()
        qc[s][3].wait_recv()
        zc[s][2].wait_recv()
        zc[s][3].wait_recv()
        project(zbuf[s, 3], s, 3)
        attend(s)
        for b in range(SIDE):
            flipped = lse[s, b].T
            lse_in[s, b, 0, 0:8] = flipped[0:8]
            lse_in[s, b, 0, 8:16] = flipped[HEAD_DIM : HEAD_DIM + 8]
        for copy in oc[s]:
            copy.start()

    for load in loads[6:]:
        load.wait()

    row = lax.broadcasted_iota(jnp.int32, (tokens, chans), 0)

    def merge_columns(left, mid, right):
        lefts = jnp.where(row == 0, 0.0, pltpu.roll(left, 1, 0))
        rights = jnp.where(row == tokens - 1, 0.0, pltpu.roll(right, tokens - 1, 0))
        return lefts + mid + rights

    def finish(s):
        for copy in oc[s]:
            copy.wait_recv()
        levels = [lse_in[s, 0, 0]] + [lse_in[s, b, 1] for b in range(1, SIDE)]
        top = functools.reduce(jnp.maximum, levels)
        scaled = [jnp.exp(level - top) for level in levels]
        inverse = 1.0 / functools.reduce(jnp.add, scaled)
        blank = jnp.zeros((HEAD_DIM - 8, tokens), F32)
        shares = [
            jnp.concatenate([(e * inverse)[0:8], blank, (e * inverse)[8:16], blank], 0).T for e in scaled
        ]
        for j in range(pairs):
            cols = slice(j * 128, (j + 1) * 128)
            total = jnp.zeros((tokens, 128), F32)
            for b in range(SIDE):
                value = part[s, 0, :, cols] if b == 0 else part_in[s, b, :, cols]
                share = jnp.where(low, shares[b][:, j : j + 1], shares[b][:, HEAD_DIM + j : HEAD_DIM + j + 1])
                total = total + share * value.astype(F32)
            att[s, :, cols] = total.astype(BF16)
        for c in range(0, chans, 128):
            cols = slice(c, c + 128)
            value = hidden[s, :, cols].astype(F32) + dot(att[s], w_out[:, cols])
            value = value.astype(BF16)
            res[s, :, cols] = value
            value = value.astype(F32)
            mean = jnp.mean(value, 0, keepdims=True)
            centred = value - mean
            gst[s, 0, 0:1, cols] = mean
            gst[s, 0, 1:2, cols] = jnp.sum(centred * centred, 0, keepdims=True)
        copies = [
            remote(gst.at[s, 0], gst.at[s, k], gsend.at[s, k - 1], grecv.at[s, k - 1], peer(k))
            for k in range(1, n_patch)
        ]
        for copy in copies:
            copy.start()
        return copies

    def group_sum(values):
        high = values.astype(BF16).astype(F32)
        rest = values - high
        mid = rest.astype(BF16).astype(F32)
        tail = rest - mid
        stack = jnp.concatenate([high, mid, tail, jnp.zeros((5, chans), F32)], 0).astype(BF16)
        sums = dot(stack, proj[...])
        return sums[0:1] + sums[1:2] + sums[2:3]

    def normalise(s, copies):
        for copy in copies:
            copy.wait_recv()
        stats = [gst[s, k] for k in range(n_patch)]
        mean = group_sum(functools.reduce(jnp.add, stats)[0:1] / n_patch) / width
        squares = jnp.zeros((1, chans), F32)
        for stat in stats:
            gap = stat[0:1] - mean
            squares = squares + (stat[1:2] + tokens * (gap * gap))
        var = group_sum(squares) / (n_patch * tokens * width)
        rate = lax.rsqrt(var + EPSILON)
        for r in range(0, tokens, 32):
            value = (res[s, r : r + 32].astype(F32) - mean) * rate
            value = value * gn_gain[...] + gn_bias[...]
            act[s, r : r + 32] = (value / (1.0 + jnp.exp(-value))).astype(BF16)
        taps = [dot(act[s], conv_w[1, b]) for b in range(3)]
        out_ref[s] = (merge_columns(*taps) + rim_sum[s] + res[s].astype(F32)).astype(BF16)

    def rim_taps():
        @pl.when(p > 0)
        def _():
            down.wait_recv()

        @pl.when(p < n_patch - 1)
        def _():
            up.wait_recv()

        for s in range(samples):
            taps = [dot(rim_near[0, s], conv_w[0, b]) + dot(rim_near[1, s], conv_w[2, b]) for b in range(3)]
            rim_sum[s] = merge_columns(*taps) + conv_b[...] + shift[s : s + 1]

    stat_copies = [finish(0)]
    rim_taps()
    stat_copies.append(finish(1))
    for s in range(samples):
        normalise(s, stat_copies[s])

    for s in range(samples):
        for copy in zc[s] + qc[s]:
            copy.wait_send()
        for copy in oc[s] + stat_copies[s]:
            copy.wait_send()

    @pl.when(p < n_patch - 1)
    def _():
        down.wait_send()

    @pl.when(p > 0)
    def _():
        up.wait_send()


def shards(
    hidden,
    stale_attn_in,
    stale_conv_in,
    ln_gain,
    ln_bias,
    w_qkv,
    w_out,
    gn_gain,
    gn_bias,
    conv_weight,
    conv_bias,
    time_shift,
):
    samples, rows, tokens, chans = hidden.shape
    block = (samples, rows * tokens, chans)
    operands = (
        hidden.reshape(block),
        stale_attn_in.reshape(block),
        stale_conv_in.reshape(block),
        ln_gain.reshape(1, chans),
        ln_bias.reshape(1, chans),
        w_qkv,
        w_out,
        gn_gain.reshape(1, chans),
        gn_bias.reshape(1, chans),
        conv_weight,
        conv_bias.reshape(1, chans),
        time_shift,
    )
    dma = pltpu.SemaphoreType.DMA
    vector = pltpu.VMEM((1, chans), F32)
    out = pl.pallas_call(
        kernel,
        out_shape=jax.ShapeDtypeStruct(block, BF16),
        in_specs=[pl.BlockSpec(memory_space=pl.ANY)] * len(operands),
        out_specs=pl.BlockSpec(memory_space=pltpu.VMEM),
        scratch_shapes=[
            pltpu.VMEM(block, BF16),
            pltpu.VMEM(block, BF16),
            pltpu.VMEM(block, BF16),
            pltpu.VMEM((2,) + block, BF16),
            vector,
            vector,
            pltpu.VMEM(w_qkv.shape, BF16),
            pltpu.VMEM(w_out.shape, BF16),
            vector,
            vector,
            pltpu.VMEM(conv_weight.shape, BF16),
            vector,
            pltpu.VMEM(time_shift.shape, F32),
            pltpu.VMEM(block, BF16),
            pltpu.VMEM((samples, SIDE, tokens, chans), BF16),
            pltpu.VMEM((samples, SIDE, tokens, chans), BF16),
            pltpu.VMEM((samples, 5 * tokens, 2 * chans), BF16),
            pltpu.VMEM((samples, SIDE, tokens, chans), BF16),
            pltpu.VMEM((samples, SIDE, tokens, chans), BF16),
            pltpu.VMEM((samples, SIDE, tokens, 128), F32),
            pltpu.VMEM((samples, SIDE, 2, 16, tokens), F32),
            pltpu.VMEM(block, BF16),
            pltpu.VMEM(block, BF16),
            pltpu.VMEM((samples, SIDE * SIDE, 2, chans), F32),
            pltpu.VMEM((chans, chans), BF16),
            pltpu.VMEM(block, F32),
            pltpu.VMEM(block, BF16),
            dma((12,)),
            dma((samples, 4)),
            dma((samples, 4)),
            dma((samples, 4)),
            dma((samples, 4)),
            dma((samples, 3, 2)),
            dma((samples, 3, 2)),
            dma((2,)),
            dma((2,)),
            dma((samples, SIDE * SIDE - 1)),
            dma((samples, SIDE * SIDE - 1)),
        ],
        compiler_params=pltpu.CompilerParams(
            collective_id=0, has_side_effects=True, vmem_limit_bytes=60 * 1024 * 1024
        ),
        name="section",
    )(*operands)
    return out.reshape(hidden.shape)


def solution(mesh):
    spread = P("img", "patch", None, None)
    return jax.shard_map(
        shards,
        mesh=mesh,
        in_specs=(spread, spread, spread) + (P(),) * 8 + (P("img", None),),
        out_specs=spread,
        check_vma=False,
    )
```

```python
import functools

import jax
import jax.numpy as jnp
from jax import lax
from jax.experimental import pallas as pl
from jax.experimental.pallas import tpu as pltpu
from jax.sharding import PartitionSpec as P

GROUPS = 32
HEAD_DIM = 64
HEAD_ROWS = 80
SIDE = 4
EPSILON = 1e-05
MESH = pl.DeviceIdType.MESH
F32 = jnp.float32
BF16 = jnp.bfloat16


def dot_nt(a, b):
    return lax.dot_general(a, b, (((1,), (1,)), ((), ())), preferred_element_type=F32)


def dot(a, b):
    return jnp.dot(a, b, preferred_element_type=F32)


def kernel(
    hidden_hbm,
    stale_hbm,
    rim_hbm,
    ln_gain_hbm,
    ln_bias_hbm,
    w_qkv_hbm,
    w_out_hbm,
    gn_gain_hbm,
    gn_bias_hbm,
    conv_w_hbm,
    conv_b_hbm,
    shift_hbm,
    out_ref,
    hidden,
    stale,
    rim_own,
    rim_near,
    rim_hop,
    ln_gain,
    ln_bias,
    w_qkv,
    w_out,
    gn_gain,
    gn_bias,
    conv_w,
    conv_b,
    shift,
    fresh,
    zbuf,
    qbuf,
    kbuf,
    w_vt,
    vt,
    scores,
    weights,
    sums,
    part,
    part_in,
    hop,
    lse,
    lse_in,
    att,
    res,
    gst,
    proj,
    rim_sum,
    act,
    load_sem,
    zsend,
    zrecv,
    qsend,
    qrecv,
    osend,
    orecv,
    hsend,
    hrecv,
    rsend,
    rrecv,
    gsend,
    grecv,
):
    n_patch = SIDE * SIDE
    samples, tokens, chans = hidden.shape
    half = tokens // 2
    p = lax.axis_index("patch")
    y, z = p // SIDE, p % SIDE
    z_next = {"patch": y * SIDE + (z + 1) % SIDE}
    z_prev = {"patch": y * SIDE + (z + SIDE - 1) % SIDE}
    y_next = {"patch": ((y + 1) % SIDE) * SIDE + z}
    y_prev = {"patch": ((y + SIDE - 1) % SIDE) * SIDE + z}
    y_far = {"patch": ((y + 2) % SIDE) * SIDE + z}

    def peer(k):
        return {"patch": (p + k) % n_patch}

    loads = []
    for i, (src, dst) in enumerate(
        (
            (stale_hbm, stale),
            (ln_gain_hbm, ln_gain),
            (ln_bias_hbm, ln_bias),
            (hidden_hbm, hidden),
            (w_qkv_hbm, w_qkv),
            (rim_hbm, rim_own),
            (w_out_hbm, w_out),
            (gn_gain_hbm, gn_gain),
            (gn_bias_hbm, gn_bias),
            (conv_b_hbm, conv_b),
            (shift_hbm, shift),
            (conv_w_hbm, conv_w),
        )
    ):
        load = pltpu.make_async_copy(src, dst, load_sem.at[i])
        load.start()
        loads.append(load)

    barrier = pltpu.get_barrier_semaphore()
    for target in (z_next, z_prev, y_next, y_prev):
        pl.semaphore_signal(barrier, inc=1, device_id=target, device_id_type=MESH)

    def remote(src, dst, send, recv, target):
        return pltpu.make_async_remote_copy(
            src_ref=src, dst_ref=dst, send_sem=send, recv_sem=recv, device_id=target, device_id_type=MESH
        )

    def ring(buf, send, recv, s, nxt, prv):
        return (
            remote(buf.at[s, 0], buf.at[s, 1], send.at[s, 0], recv.at[s, 0], nxt),
            remote(buf.at[s, 0], buf.at[s, 2], send.at[s, 1], recv.at[s, 1], prv),
            remote(
                buf.at[s, 1, pl.ds(0, half)], buf.at[s, 3, pl.ds(0, half)], send.at[s, 2], recv.at[s, 2], nxt
            ),
            remote(
                buf.at[s, 2, pl.ds(half, half)],
                buf.at[s, 3, pl.ds(half, half)],
                send.at[s, 3],
                recv.at[s, 3],
                prv,
            ),
        )

    zc = [ring(zbuf, zsend, zrecv, s, z_next, z_prev) for s in range(samples)]
    qc = [ring(qbuf, qsend, qrecv, s, y_next, y_prev) for s in range(samples)]

    def layer_norm(values):
        values = values.astype(F32)
        centre = jnp.mean(values, -1, keepdims=True)
        centred = values - centre
        spread = jnp.mean(centred * centred, -1, keepdims=True)
        return (centred * lax.rsqrt(spread + EPSILON) * ln_gain[...].reshape(1, chans) + ln_bias[...].reshape(1, chans)).astype(BF16)

    step = 32
    def norm_stale(s):
        with jax.named_scope("norm_stale"):

            @pl.loop(0, tokens // step)
            def _(i):
                rows = pl.ds(pl.multiple_of(i * step, step), step)
                zbuf[s, 0, rows] = layer_norm(stale[s, rows])

    for load in loads[:3]:
        load.wait()
    norm_stale(0)
    with jax.named_scope("barrier"):
        pl.semaphore_wait(barrier, 4)
    for s in range(samples):
        if s > 0:
            norm_stale(s)
        zc[s][0].start()
        zc[s][1].start()

    with jax.named_scope("norm_fresh"):
        loads[3].wait()
        for s in range(samples):

            @pl.loop(0, tokens // step)
            def _(i):
                rows = pl.ds(pl.multiple_of(i * step, step), step)
                fresh[s, rows] = layer_norm(hidden[s, rows])

    with jax.named_scope("turn_weights"):
        lse[...] = jnp.zeros(lse.shape, F32)
        loads[4].wait()
        for r in range(0, chans, 128):
            for c in range(0, chans, 128):
                block = w_qkv[r : r + 128, 2 * chans + c : 2 * chans + c + 128]
                w_vt[c : c + 128, r : r + 128] = block.astype(F32).T.astype(BF16)
        for u in range(2):
            weights[2 * u, 3 * tokens :, :tokens] = jnp.zeros((tokens, tokens), BF16)
            weights[2 * u, :tokens, tokens:] = jnp.zeros((tokens, tokens), BF16)

    with jax.named_scope("queries"):
        for s in range(samples):
            for c in range(0, chans, 128):
                q = dot(fresh[s], w_qkv[:, c : c + 128]).astype(BF16)
                qbuf[s, 0, :, c : c + 128] = q * BF16(HEAD_DIM**-0.5)
            qc[s][0].start()
            qc[s][1].start()

    heads = chans // HEAD_DIM

    def project(src, s, block, count):
        rows = slice(block * tokens, (block + count) * tokens)
        for c in range(0, chans, 128):
            kbuf[s, rows, c : c + 128] = dot(src, w_qkv[:, chans + c : chans + c + 128]).astype(BF16)
        values = dot_nt(w_vt[...], src).astype(BF16)
        for h in range(heads):
            vt[s, h * HEAD_ROWS : h * HEAD_ROWS + HEAD_DIM, rows] = values[h * HEAD_DIM : (h + 1) * HEAD_DIM]

    with jax.named_scope("own_pairs"):
        for s in range(samples):
            project(fresh[s], s, 0, 1)
            project(zbuf[s, 0], s, 3, 1)
            for h in range(heads):
                vt[s, h * HEAD_ROWS + HEAD_DIM : (h + 1) * HEAD_ROWS, :] = jnp.ones(
                    (HEAD_ROWS - HEAD_DIM, 5 * tokens), BF16
                )

    width = chans // GROUPS

    def group_of(v):
        return (v * (65536 // width + 1)) >> 16

    for r in range(0, chans, 128):
        same = group_of(lax.broadcasted_iota(jnp.int32, (128, chans), 0) + r) == group_of(
            lax.broadcasted_iota(jnp.int32, (128, chans), 1)
        )
        proj[r : r + 128] = jnp.where(same, 1.0, 0.0).astype(BF16)

    keys = 3 * tokens
    pairs = chans // 128
    low = lax.broadcasted_iota(jnp.int32, (2 * tokens, 128), 1) < HEAD_DIM
    units = [(head, t) for head in range(heads) for t in range(2)]

    def masked_queries(s, head, t):
        cols = slice(head // 2 * 128, head // 2 * 128 + 128)
        queries = qbuf[s, 2 * t : 2 * t + 2, :, cols].reshape(2 * tokens, 128)
        return cols, jnp.where(low if head % 2 == 0 else ~low, queries, BF16(0))

    def attend_near(s):
        peaks = {}

        def score(i):
            head, t = units[i]
            u = i % 4
            first = 0 if t == 0 else tokens
            cols, queries = masked_queries(s, head, t)
            value = dot_nt(kbuf[s, first : 4 * tokens, cols], queries)
            if t == 0:
                scores[u] = value
                peaks[i] = (
                    jnp.max(value[:keys, :tokens], 0, keepdims=True),
                    jnp.max(value[tokens:, tokens:], 0, keepdims=True),
                )
            else:
                scores[u, tokens:] = value
                top = jnp.max(value, 0, keepdims=True)
                peaks[i] = (top[:, :tokens], top[:, tokens:])

        def apply(i):
            head, t = units[i]
            u = i % 4
            for half, top in enumerate(peaks[i]):
                lanes = slice(half * tokens, (half + 1) * tokens)
                first = 0 if t == 0 and half == 0 else tokens
                rows = slice(first, first + keys)
                weights[u, rows, lanes] = jnp.exp(scores[u, rows, lanes] - top).astype(BF16)
            mine = slice(head * HEAD_ROWS, (head + 1) * HEAD_ROWS)
            first = 0 if t == 0 else tokens
            sums[s, t, mine] = dot(vt[s, mine, first : 4 * tokens], weights[u, first:])
            spare = slice(head * HEAD_ROWS + HEAD_DIM + 8, (head + 1) * HEAD_ROWS)
            sums[s, t, spare] = jnp.broadcast_to(jnp.concatenate(peaks[i], 1), (8, 2 * tokens))

        ahead = 2
        for i in range(len(units) + ahead):
            if i < len(units):
                score(i)
            if i >= ahead:
                apply(i - ahead)

    def attend_far(s, heads_of):
        values, gains = {}, {}
        mine = [unit for unit in units if unit[0] in heads_of]

        def score(i):
            head, t = mine[i]
            cols, queries = masked_queries(s, head, t)
            values[i] = dot_nt(kbuf[s, 4 * tokens :, cols], queries)

        def weigh(i):
            head, t = mine[i]
            spare = slice(head * HEAD_ROWS + HEAD_DIM + 8, (head + 1) * HEAD_ROWS)
            before = sums[s, t, spare][0:1]
            top = jnp.maximum(before, jnp.max(values[i], 0, keepdims=True))
            gains[i] = (jnp.exp(before - top), top)
            values[i] = jnp.exp(values[i] - top).astype(BF16)

        def apply(i):
            head, t = mine[i]
            gain, top = gains[i]
            rows = slice(head * HEAD_ROWS, (head + 1) * HEAD_ROWS)
            total = sums[s, t, rows] * gain + dot(vt[s, rows, 4 * tokens :], values[i])
            norm = total[HEAD_DIM : HEAD_DIM + 1]
            ratio = (total[:HEAD_DIM] * (1.0 / norm)).astype(BF16)
            level = top + jnp.log(norm)
            for half in range(2):
                lanes = slice(half * tokens, (half + 1) * tokens)
                b = 2 * t + half
                part[s, b, head * HEAD_DIM : (head + 1) * HEAD_DIM] = ratio[:, lanes]
                lse[s, b, head : head + 1] = level[:, lanes]

        for i in range(len(mine) + 2):
            if i < len(mine):
                score(i)
            if 0 <= i - 1 < len(mine):
                weigh(i - 1)
            if 0 <= i - 2 < len(mine):
                apply(i - 2)

    upper, lower = pl.ds(0, chans // 2), pl.ds(chans // 2, chans // 2)
    hops, relays, oc = [], [], []
    for s in range(samples):
        hops.append(
            (
                remote(part.at[s, 3, upper], hop.at[s, 0], hsend.at[s, 0], hrecv.at[s, 0], y_next),
                remote(part.at[s, 3, lower], hop.at[s, 1], hsend.at[s, 1], hrecv.at[s, 1], y_prev),
            )
        )
        relays.append(
            (
                remote(hop.at[s, 0], part_in.at[s, 3, upper], hsend.at[s, 2], hrecv.at[s, 2], y_next),
                remote(hop.at[s, 1], part_in.at[s, 3, lower], hsend.at[s, 3], hrecv.at[s, 3], y_prev),
            )
        )
        copies = ([], [])
        for i, (b, there, target) in enumerate(((1, 2, y_prev), (2, 1, y_next), (3, 3, y_far))):
            if b < 3:
                for n, rows in enumerate((upper, lower)):
                    copies[n].append(
                        remote(
                            part.at[s, b, rows],
                            part_in.at[s, there, rows],
                            osend.at[s, i, n],
                            orecv.at[s, there - 1, n],
                            target,
                        )
                    )
            copies[1].append(
                remote(lse.at[s, b], lse_in.at[s, there], osend.at[s, i, 2], orecv.at[s, there - 1, 2], target)
            )
        oc.append(copies)

    def send_parts(s, n):
        hops[s][n].start()
        for copy in oc[s][n]:
            copy.start()

    def relay_parts(s):
        with jax.named_scope("wait_hops"):
            for copy, onward in zip(hops[s], relays[s]):
                copy.wait_recv()
                onward.start()

    def near(s):
        with jax.named_scope("wait_q_near"):
            qc[s][0].wait_recv()
            qc[s][2].start()
            qc[s][1].wait_recv()
            qc[s][3].start()
        with jax.named_scope("wait_z_near"):
            zc[s][0].wait_recv()
            zc[s][2].start()
            zc[s][1].wait_recv()
            zc[s][3].start()
        with jax.named_scope("near_pairs"):
            project(zbuf[s, 1:3].reshape(2 * tokens, chans), s, 1, 2)

    def far(s):
        with jax.named_scope("wait_z_far"):
            zc[s][2].wait_recv()
            zc[s][3].wait_recv()
        if s == samples - 1:
            start_rims()
        with jax.named_scope("far_pairs"):
            project(zbuf[s, 3], s, 4, 1)
        for n in range(2):
            with jax.named_scope("attend_far"):
                attend_far(s, range(n * heads // 2, (n + 1) * heads // 2))
            send_parts(s, n)

    def wait_far_queries(s):
        with jax.named_scope("wait_q_far"):
            qc[s][2].wait_recv()
            qc[s][3].wait_recv()

    above, below = rim_near.at[0], rim_near.at[1]
    last, gone = SIDE - 1, n_patch - 1
    across = (
        remote(rim_own, rim_hop, rsend.at[2], rrecv.at[2], y_next),
        remote(rim_own, rim_hop, rsend.at[2], rrecv.at[2], y_prev),
    )
    down = [remote(rim, above, rsend.at[0], rrecv.at[0], z_next) for rim in (rim_own, rim_hop)]
    up = [remote(rim, below, rsend.at[1], rrecv.at[1], z_prev) for rim in (rim_own, rim_hop)]
    sends_across = (jnp.logical_and(z == last, y < last), jnp.logical_and(z == 0, y > 0))
    gets_across = jnp.logical_or(jnp.logical_and(z == last, y > 0), jnp.logical_and(z == 0, y < last))
    sends_down = (z < last, jnp.logical_and(z == last, y > 0))
    sends_up = (z > 0, jnp.logical_and(z == 0, y < last))

    def start_rims_across():
        loads[5].wait()
        for condition, copy in zip(sends_across, across):
            pl.when(condition)(copy.start)

    def start_rims():
        pl.when(gets_across)(across[0].wait_recv)
        for conditions, copies in ((sends_down, down), (sends_up, up)):
            for condition, copy in zip(conditions, copies):
                pl.when(condition)(copy.start)

        @pl.when(p == 0)
        def _():
            rim_near[0] = jnp.zeros(rim_near.shape[1:], BF16)

        @pl.when(p == gone)
        def _():
            rim_near[1] = jnp.zeros(rim_near.shape[1:], BF16)

    near(0)
    wait_far_queries(0)
    with jax.named_scope("attend_near"):
        attend_near(0)
    near(1)

    start_rims_across()
    wait_far_queries(1)
    far(0)
    with jax.named_scope("attend_near"):
        attend_near(1)
    relay_parts(0)
    far(1)

    with jax.named_scope("wait_loads"):
        for load in loads[6:]:
            load.wait()

    row = lax.broadcasted_iota(jnp.int32, (tokens, chans), 0)

    def merge_columns(left, mid, right):
        lefts = jnp.where(row == 0, 0.0, pltpu.roll(left, 1, 0))
        rights = jnp.where(row == tokens - 1, 0.0, pltpu.roll(right, tokens - 1, 0))
        return lefts + mid + rights

    def finish(s):
        with jax.named_scope("wait_parts"):
            for copy in oc[s][0] + oc[s][1] + list(relays[s]):
                copy.wait_recv()
        with jax.named_scope("merge"):
            levels = [lse[s, 0]] + [lse_in[s, b] for b in range(1, SIDE)]
            top = functools.reduce(jnp.maximum, levels)
            scaled = [jnp.exp(level - top) for level in levels]
            inverse = 1.0 / functools.reduce(jnp.add, scaled)
            shares = [e * inverse for e in scaled]
            for j in range(pairs):
                totals = []
                for h in (2 * j, 2 * j + 1):
                    rows = slice(h * HEAD_DIM, (h + 1) * HEAD_DIM)
                    total = shares[0][h : h + 1] * part[s, 0, rows].astype(F32)
                    for b in range(1, SIDE):
                        total = total + shares[b][h : h + 1] * part_in[s, b, rows].astype(F32)
                    totals.append(total)
                att[s, :, j * 128 : (j + 1) * 128] = jnp.concatenate(totals, 0).T.astype(BF16)
        with jax.named_scope("out_proj"):
            for c in range(0, chans, 128):
                cols = slice(c, c + 128)
                value = hidden[s, :, cols].astype(F32) + dot(att[s], w_out[:, cols])
                value = value.astype(BF16)
                res[s, :, cols] = value
                value = value.astype(F32)
                mean = jnp.mean(value, 0, keepdims=True)
                centred = value - mean
                gst[s, 0, 0:1, cols] = mean
                gst[s, 0, 1:2, cols] = jnp.sum(centred * centred, 0, keepdims=True)
        copies = [
            remote(gst.at[s, 0], gst.at[s, k], gsend.at[s, k - 1], grecv.at[s, k - 1], peer(k))
            for k in range(1, n_patch)
        ]
        for copy in copies:
            copy.start()
        return copies

    def group_sum(values):
        high = values.astype(BF16).astype(F32)
        rest = values - high
        mid = rest.astype(BF16).astype(F32)
        tail = rest - mid
        stack = jnp.concatenate([high, mid, tail, jnp.zeros((5, chans), F32)], 0).astype(BF16)
        sums = dot(stack, proj[...])
        return sums[0:1] + sums[1:2] + sums[2:3]

    def normalise(s, copies):
        with jax.named_scope("wait_stats"):
            for copy in copies:
                copy.wait_recv()
        with jax.named_scope("stats"):
            stats = [gst[s, k] for k in range(n_patch)]
            mean = group_sum(functools.reduce(jnp.add, stats)[0:1] / n_patch) / width
            squares = jnp.zeros((1, chans), F32)
            for stat in stats:
                gap = stat[0:1] - mean
                squares = squares + (stat[1:2] + tokens * (gap * gap))
            var = group_sum(squares) / (n_patch * tokens * width)
            rate = lax.rsqrt(var + EPSILON)
        with jax.named_scope("silu"):
            for r in range(0, tokens, 32):
                value = (res[s, r : r + 32].astype(F32) - mean) * rate
                value = value * gn_gain[...].reshape(1, chans) + gn_bias[...].reshape(1, chans)
                act[s, r : r + 32] = (value / (1.0 + jnp.exp(-value))).astype(BF16)
        with jax.named_scope("conv"):
            taps = [dot(act[s], conv_w[1, b]) for b in range(3)]
            out_ref[s] = (merge_columns(*taps) + rim_sum[s] + res[s].astype(F32)).astype(BF16)

    def rim_taps():
        with jax.named_scope("wait_rims"):
            pl.when(p > 0)(down[0].wait_recv)
            pl.when(p < gone)(up[0].wait_recv)

        with jax.named_scope("rim_taps"):
            for s in range(samples):
                taps = [dot(rim_near[0, s], conv_w[0, b]) + dot(rim_near[1, s], conv_w[2, b]) for b in range(3)]
                rim_sum[s] = merge_columns(*taps) + conv_b[...].reshape(1, chans) + shift[s : s + 1]

    stat_copies = [finish(0)]
    relay_parts(1)
    stat_copies.append(finish(1))
    rim_taps()
    normalise(0, stat_copies[0])
    normalise(1, stat_copies[1])

    for s in range(samples):
        for copy in zc[s] + qc[s]:
            copy.wait_send()
        for copy in oc[s][0] + oc[s][1] + list(hops[s] + relays[s]) + stat_copies[s]:
            copy.wait_send()

    for condition, copy in zip(sends_across, across):
        pl.when(condition)(copy.wait_send)
    for conditions, copies in ((sends_down, down), (sends_up, up)):
        for condition, copy in zip(conditions, copies):
            pl.when(condition)(copy.wait_send)


def shards(
    hidden,
    stale_attn_in,
    stale_conv_in,
    ln_gain,
    ln_bias,
    w_qkv,
    w_out,
    gn_gain,
    gn_bias,
    conv_weight,
    conv_bias,
    time_shift,
):
    samples, rows, tokens, chans = hidden.shape
    block = (samples, rows * tokens, chans)
    operands = (
        hidden.reshape(block),
        stale_attn_in.reshape(block),
        stale_conv_in.reshape(block),
        ln_gain,
        ln_bias,
        w_qkv,
        w_out,
        gn_gain,
        gn_bias,
        conv_weight,
        conv_bias,
        time_shift,
    )
    dma = pltpu.SemaphoreType.DMA
    vector = pltpu.VMEM((chans,), F32)
    out = pl.pallas_call(
        kernel,
        out_shape=jax.ShapeDtypeStruct(block, BF16),
        in_specs=[pl.BlockSpec(memory_space=pl.ANY)] * len(operands),
        out_specs=pl.BlockSpec(memory_space=pltpu.VMEM),
        scratch_shapes=[
            pltpu.VMEM(block, BF16),
            pltpu.VMEM(block, BF16),
            pltpu.VMEM(block, BF16),
            pltpu.VMEM((2,) + block, BF16),
            pltpu.VMEM(block, BF16),
            vector,
            vector,
            pltpu.VMEM(w_qkv.shape, BF16),
            pltpu.VMEM(w_out.shape, BF16),
            vector,
            vector,
            pltpu.VMEM(conv_weight.shape, BF16),
            vector,
            pltpu.VMEM(time_shift.shape, F32),
            pltpu.VMEM(block, BF16),
            pltpu.VMEM((samples, SIDE, tokens, chans), BF16),
            pltpu.VMEM((samples, SIDE, tokens, chans), BF16),
            pltpu.VMEM((samples, 5 * tokens, chans), BF16),
            pltpu.VMEM((chans, chans), BF16),
            pltpu.VMEM((samples, chans // HEAD_DIM * HEAD_ROWS, 5 * tokens), BF16),
            pltpu.VMEM((4, 4 * tokens, 2 * tokens), F32),
            pltpu.VMEM((4, 4 * tokens, 2 * tokens), BF16),
            pltpu.VMEM((samples, 2, chans // HEAD_DIM * HEAD_ROWS, 2 * tokens), F32),
            pltpu.VMEM((samples, SIDE, chans, tokens), BF16),
            pltpu.VMEM((samples, SIDE, chans, tokens), BF16),
            pltpu.VMEM((samples, 2, chans // 2, tokens), BF16),
            pltpu.VMEM((samples, SIDE, 16, tokens), F32),
            pltpu.VMEM((samples, SIDE, 16, tokens), F32),
            pltpu.VMEM(block, BF16),
            pltpu.VMEM(block, BF16),
            pltpu.VMEM((samples, SIDE * SIDE, 2, chans), F32),
            pltpu.VMEM((chans, chans), BF16),
            pltpu.VMEM(block, F32),
            pltpu.VMEM(block, BF16),
            dma((12,)),
            dma((samples, 4)),
            dma((samples, 4)),
            dma((samples, 4)),
            dma((samples, 4)),
            dma((samples, 3, 3)),
            dma((samples, 3, 3)),
            dma((samples, 4)),
            dma((samples, 4)),
            dma((3,)),
            dma((3,)),
            dma((samples, SIDE * SIDE - 1)),
            dma((samples, SIDE * SIDE - 1)),
        ],
        compiler_params=pltpu.CompilerParams(
            collective_id=0, has_side_effects=True, vmem_limit_bytes=60 * 1024 * 1024
        ),
        name="section",
    )(*operands)
    return out.reshape(hidden.shape)


def solution(mesh):
    spread = P("img", "patch", None, None)
    return jax.shard_map(
        shards,
        mesh=mesh,
        in_specs=(spread, spread, spread) + (P(),) * 8 + (P("img", None),),
        out_specs=spread,
        check_vma=False,
    )
```

```python
import functools

import jax
import jax.numpy as jnp
from jax import lax
from jax.experimental import pallas as pl
from jax.experimental.pallas import tpu as pltpu
from jax.sharding import PartitionSpec as P

GROUPS = 32
HEAD_DIM = 64
HEAD_ROWS = 80
SIDE = 4
EPSILON = 1e-05
MESH = pl.DeviceIdType.MESH
F32 = jnp.float32
BF16 = jnp.bfloat16


def dot_nt(a, b):
    return lax.dot_general(a, b, (((1,), (1,)), ((), ())), preferred_element_type=F32)


def dot(a, b):
    return jnp.dot(a, b, preferred_element_type=F32)


def kernel(
    hidden_hbm,
    stale_hbm,
    rim_hbm,
    ln_gain_hbm,
    ln_bias_hbm,
    w_qkv_hbm,
    w_out_hbm,
    gn_gain_hbm,
    gn_bias_hbm,
    conv_w_hbm,
    conv_b_hbm,
    shift_hbm,
    out_hbm,
    hidden,
    stale,
    rim_own,
    rim_near,
    rim_hop,
    ln_gain,
    ln_bias,
    w_qkv,
    w_out,
    gn_gain,
    gn_bias,
    conv_w,
    conv_b,
    shift,
    fresh,
    zbuf,
    qbuf,
    kbuf,
    w_vt,
    vt,
    scores,
    weights,
    sums,
    part,
    part_in,
    hop,
    lse,
    lse_in,
    lse_hop,
    att,
    res,
    gst,
    proj,
    rim_sum,
    act,
    out,
    load_sem,
    out_sem,
    zsend,
    zrecv,
    qsend,
    qrecv,
    osend,
    orecv,
    rsend,
    rrecv,
    gsend,
    grecv,
):
    n_patch = SIDE * SIDE
    samples, tokens, chans = hidden.shape
    half = tokens // 2
    p = lax.axis_index("patch")
    y, z = p // SIDE, p % SIDE
    z_next = {"patch": y * SIDE + (z + 1) % SIDE}
    z_prev = {"patch": y * SIDE + (z + SIDE - 1) % SIDE}
    y_next = {"patch": ((y + 1) % SIDE) * SIDE + z}
    y_prev = {"patch": ((y + SIDE - 1) % SIDE) * SIDE + z}

    def peer(k):
        return {"patch": (p + k) % n_patch}

    loads = []
    for i, (src, dst) in enumerate(
        (
            (stale_hbm, stale),
            (ln_gain_hbm, ln_gain),
            (ln_bias_hbm, ln_bias),
            (hidden_hbm, hidden),
            (w_qkv_hbm, w_qkv),
            (rim_hbm, rim_own),
            (w_out_hbm, w_out),
            (gn_gain_hbm, gn_gain),
            (gn_bias_hbm, gn_bias),
            (conv_b_hbm, conv_b),
            (shift_hbm, shift),
            (conv_w_hbm, conv_w),
        )
    ):
        load = pltpu.make_async_copy(src, dst, load_sem.at[i])
        load.start()
        loads.append(load)

    barrier = pltpu.get_barrier_semaphore()
    for target in (z_next, z_prev, y_next, y_prev):
        pl.semaphore_signal(barrier, inc=1, device_id=target, device_id_type=MESH)

    def remote(src, dst, send, recv, target):
        return pltpu.make_async_remote_copy(
            src_ref=src, dst_ref=dst, send_sem=send, recv_sem=recv, device_id=target, device_id_type=MESH
        )

    def ring(buf, send, recv, s, nxt, prv):
        return (
            remote(buf.at[s, 0], buf.at[s, 1], send.at[s, 0], recv.at[s, 0], nxt),
            remote(buf.at[s, 0], buf.at[s, 2], send.at[s, 1], recv.at[s, 1], prv),
            remote(
                buf.at[s, 1, pl.ds(0, half)], buf.at[s, 3, pl.ds(0, half)], send.at[s, 2], recv.at[s, 2], nxt
            ),
            remote(
                buf.at[s, 2, pl.ds(half, half)],
                buf.at[s, 3, pl.ds(half, half)],
                send.at[s, 3],
                recv.at[s, 3],
                prv,
            ),
        )

    zc = [ring(zbuf, zsend, zrecv, s, z_next, z_prev) for s in range(samples)]
    qc = [ring(qbuf, qsend, qrecv, s, y_next, y_prev) for s in range(samples)]

    def layer_norm(values):
        values = values.astype(F32)
        centre = jnp.mean(values, -1, keepdims=True)
        centred = values - centre
        spread = jnp.mean(centred * centred, -1, keepdims=True)
        return (centred * lax.rsqrt(spread + EPSILON) * ln_gain[...].reshape(1, chans) + ln_bias[...].reshape(1, chans)).astype(BF16)

    step = 32
    blocks = [slice(c, min(c + 256, chans)) for c in range(0, chans, 256)]
    def norm_stale(s):
        with jax.named_scope("norm_stale"):

            @pl.loop(0, tokens // step, unroll=True)
            def _(i):
                rows = pl.ds(pl.multiple_of(i * step, step), step)
                zbuf[s, 0, rows] = layer_norm(stale[s, rows])

    for load in loads[:3]:
        load.wait()
    norm_stale(0)
    with jax.named_scope("barrier"):
        pl.semaphore_wait(barrier, 4)
    for s in range(samples):
        if s > 0:
            norm_stale(s)
        zc[s][0].start()
        zc[s][1].start()

    with jax.named_scope("norm_fresh"):
        loads[3].wait()
        for s in range(samples):

            @pl.loop(0, tokens // step, unroll=True)
            def _(i):
                rows = pl.ds(pl.multiple_of(i * step, step), step)
                fresh[s, rows] = layer_norm(hidden[s, rows])

    with jax.named_scope("turn_weights"):
        lse[...] = jnp.zeros(lse.shape, F32)
        loads[4].wait()
        for r in range(0, chans, 128):
            for c in range(0, chans, 128):
                block = w_qkv[r : r + 128, 2 * chans + c : 2 * chans + c + 128]
                w_vt[c : c + 128, r : r + 128] = block.astype(F32).T.astype(BF16)
        for u in range(2):
            weights[2 * u, 3 * tokens :, :tokens] = jnp.zeros((tokens, tokens), BF16)
            weights[2 * u, :tokens, tokens:] = jnp.zeros((tokens, tokens), BF16)

    with jax.named_scope("queries"):
        for s in range(samples):
            for cols in blocks:
                q = dot(fresh[s], w_qkv[:, cols]).astype(BF16)
                qbuf[s, 0, :, cols] = q * BF16(HEAD_DIM**-0.5)
            qc[s][0].start()
            qc[s][1].start()

    heads = chans // HEAD_DIM

    def project(src, s, block, count):
        rows = slice(block * tokens, (block + count) * tokens)
        for cols in blocks:
            kbuf[s, rows, cols] = dot(src, w_qkv[:, chans + cols.start : chans + cols.stop]).astype(BF16)
        values = dot_nt(w_vt[...], src).astype(BF16)
        for h in range(heads):
            vt[s, h * HEAD_ROWS : h * HEAD_ROWS + HEAD_DIM, rows] = values[h * HEAD_DIM : (h + 1) * HEAD_DIM]

    with jax.named_scope("own_pairs"):
        for s in range(samples):
            project(fresh[s], s, 0, 1)
            project(zbuf[s, 0], s, 3, 1)
            for h in range(heads):
                vt[s, h * HEAD_ROWS + HEAD_DIM : (h + 1) * HEAD_ROWS, :] = jnp.ones(
                    (HEAD_ROWS - HEAD_DIM, 5 * tokens), BF16
                )

    width = chans // GROUPS

    def group_of(v):
        return (v * (65536 // width + 1)) >> 16

    for r in range(0, chans, 128):
        same = group_of(lax.broadcasted_iota(jnp.int32, (128, chans), 0) + r) == group_of(
            lax.broadcasted_iota(jnp.int32, (128, chans), 1)
        )
        proj[r : r + 128] = jnp.where(same, 1.0, 0.0).astype(BF16)

    keys = 3 * tokens
    pairs = chans // 128
    low = lax.broadcasted_iota(jnp.int32, (2 * tokens, 128), 1) < HEAD_DIM
    units = [(head, t) for head in range(heads) for t in range(2)]

    def masked_queries(s, head, t):
        cols = slice(head // 2 * 128, head // 2 * 128 + 128)
        queries = qbuf[s, 2 * t : 2 * t + 2, :, cols].reshape(2 * tokens, 128)
        return cols, jnp.where(low if head % 2 == 0 else ~low, queries, BF16(0))

    def attend_near(s, units):
        peaks = {}

        def score(i):
            head, t = units[i]
            u = i % 4
            first = 0 if t == 0 else tokens
            cols, queries = masked_queries(s, head, t)
            value = dot_nt(kbuf[s, first : 4 * tokens, cols], queries)
            if t == 0:
                scores[u] = value
                peaks[i] = (
                    jnp.max(value[:keys, :tokens], 0, keepdims=True),
                    jnp.max(value[tokens:, tokens:], 0, keepdims=True),
                )
            else:
                scores[u, tokens:] = value
                top = jnp.max(value, 0, keepdims=True)
                peaks[i] = (top[:, :tokens], top[:, tokens:])

        def apply(i):
            head, t = units[i]
            u = i % 4
            for half, top in enumerate(peaks[i]):
                lanes = slice(half * tokens, (half + 1) * tokens)
                first = 0 if t == 0 and half == 0 else tokens
                rows = slice(first, first + keys)
                weights[u, rows, lanes] = jnp.exp(scores[u, rows, lanes] - top).astype(BF16)
            mine = slice(head * HEAD_ROWS, (head + 1) * HEAD_ROWS)
            first = 0 if t == 0 else tokens
            sums[s, t, mine] = dot(vt[s, mine, first : 4 * tokens], weights[u, first:])
            spare = slice(head * HEAD_ROWS + HEAD_DIM + 8, (head + 1) * HEAD_ROWS)
            sums[s, t, spare] = jnp.broadcast_to(jnp.concatenate(peaks[i], 1), (8, 2 * tokens))

        ahead = 3
        for i in range(len(units) + ahead):
            if i < len(units):
                score(i)
            if i >= ahead:
                apply(i - ahead)

    def attend_far(s, mine):
        values, gains = {}, {}

        def score(i):
            head, t = mine[i]
            cols, queries = masked_queries(s, head, t)
            values[i] = dot_nt(kbuf[s, 4 * tokens :, cols], queries)

        def weigh(i):
            head, t = mine[i]
            spare = slice(head * HEAD_ROWS + HEAD_DIM + 8, (head + 1) * HEAD_ROWS)
            before = sums[s, t, spare][0:1]
            top = jnp.maximum(before, jnp.max(values[i], 0, keepdims=True))
            gains[i] = (jnp.exp(before - top), top)
            values[i] = jnp.exp(values[i] - top).astype(BF16)

        def apply(i):
            head, t = mine[i]
            gain, top = gains[i]
            rows = slice(head * HEAD_ROWS, (head + 1) * HEAD_ROWS)
            total = sums[s, t, rows] * gain + dot(vt[s, rows, 4 * tokens :], values[i])
            norm = total[HEAD_DIM : HEAD_DIM + 1]
            ratio = (total[:HEAD_DIM] * (1.0 / norm)).astype(BF16)
            level = top + jnp.log(norm)
            for half in range(2):
                lanes = slice(half * tokens, (half + 1) * tokens)
                b = 2 * t + half
                part[s, b, head * HEAD_DIM : (head + 1) * HEAD_DIM] = ratio[:, lanes]
                lse[s, b, head : head + 1] = level[:, lanes]

        for i in range(len(mine) + 2):
            if i < len(mine):
                score(i)
            if 0 <= i - 1 < len(mine):
                weigh(i - 1)
            if 0 <= i - 2 < len(mine):
                apply(i - 2)

    upper, lower = pl.ds(0, chans // 2), pl.ds(chans // 2, chans // 2)
    hops, plain, merged = [], [], []
    for s in range(samples):

        def to(i, src, dst, target):
            return remote(src, dst, osend.at[s, i], orecv.at[s, i], target)

        hops.append(
            (
                (to(0, part.at[s, 3, upper], hop.at[s, 0], y_next), to(2, lse.at[s, 3], lse_hop.at[s, 0], y_next)),
                (to(1, part.at[s, 3, lower], hop.at[s, 1], y_prev), to(3, lse.at[s, 3], lse_hop.at[s, 1], y_prev)),
            )
        )
        plain.append(
            (
                to(4, part.at[s, 1, upper], part_in.at[s, 1, upper], y_prev),
                to(5, part.at[s, 2, lower], part_in.at[s, 0, lower], y_next),
            )
        )
        merged.append(
            (
                (to(6, part.at[s, 2, upper], part_in.at[s, 0, upper], y_next), to(8, lse.at[s, 2], lse_in.at[s, 0], y_next)),
                (to(7, part.at[s, 1, lower], part_in.at[s, 1, lower], y_prev), to(9, lse.at[s, 1], lse_in.at[s, 1], y_prev)),
            )
        )

    def send_parts(s, n):
        if n < 2:
            hops[s][n][0].start()
        if n == 1:
            hops[s][0][1].start()
            hops[s][1][1].start()
            plain[s][1].start()
        if n == 2:
            plain[s][0].start()

    def relay_parts(s):
        for n, b in ((0, 2), (1, 1)):
            with jax.named_scope("wait_hops"):
                for copy in hops[s][n]:
                    copy.wait_recv()
            with jax.named_scope("add_hops"):
                near_level, far_level = lse[s, b], lse_hop[s, n]
                top = jnp.maximum(near_level, far_level)
                near_scale, far_scale = jnp.exp(near_level - top), jnp.exp(far_level - top)
                total = near_scale + far_scale
                near_scale, far_scale = near_scale / total, far_scale / total
                first = n * heads // 2
                for h in range(first, first + heads // 2):
                    rows = slice(h * HEAD_DIM, (h + 1) * HEAD_DIM)
                    there = slice((h - first) * HEAD_DIM, (h - first + 1) * HEAD_DIM)
                    value = near_scale[h : h + 1] * part[s, b, rows].astype(F32)
                    value = value + far_scale[h : h + 1] * hop[s, n, there].astype(F32)
                    part[s, b, rows] = value.astype(BF16)
                lse[s, b, first : first + heads // 2] = (top + jnp.log(total))[first : first + heads // 2]
            for copy in merged[s][n]:
                copy.start()

    def near_queries(s):
        with jax.named_scope("wait_q_near"):
            qc[s][0].wait_recv()
            qc[s][2].start()
            qc[s][1].wait_recv()
            qc[s][3].start()

    def near_keys(s):
        with jax.named_scope("wait_z_near"):
            zc[s][0].wait_recv()
            zc[s][2].start()
            zc[s][1].wait_recv()
            zc[s][3].start()
        with jax.named_scope("near_pairs"):
            project(zbuf[s, 1:3].reshape(2 * tokens, chans), s, 1, 2)

    def far(s):
        with jax.named_scope("wait_z_far"):
            zc[s][2].wait_recv()
            zc[s][3].wait_recv()
        with jax.named_scope("far_pairs"):
            project(zbuf[s, 3], s, 4, 1)
        first, second = range(heads // 2), range(heads // 2, heads)
        for n, mine in enumerate(([(h, 1) for h in first], [(h, 1) for h in second], [(h, 0) for h in range(heads)])):
            with jax.named_scope("attend_far"):
                attend_far(s, mine)
            send_parts(s, n)

    def wait_far_queries(s):
        with jax.named_scope("wait_q_far"):
            qc[s][2].wait_recv()
            qc[s][3].wait_recv()

    last, gone = SIDE - 1, n_patch - 1
    sends_across = (jnp.logical_and(z == last, y < last), jnp.logical_and(z == 0, y > 0))
    gets_across = jnp.logical_or(jnp.logical_and(z == last, y > 0), jnp.logical_and(z == 0, y < last))
    sends_down = (z < last, jnp.logical_and(z == last, y > 0))
    sends_up = (z > 0, jnp.logical_and(z == 0, y < last))
    across, down, up = [], [], []
    for s in range(samples):

        def rim(i, src, dst, target):
            return remote(src.at[s], dst.at[s], rsend.at[s, i], rrecv.at[s, i], target)

        across.append([rim(2, rim_own, rim_hop, target) for target in (y_next, y_prev)])
        down.append([rim(0, src, rim_near.at[0], z_next) for src in (rim_own, rim_hop)])
        up.append([rim(1, src, rim_near.at[1], z_prev) for src in (rim_own, rim_hop)])

    def start_rims_across():
        loads[5].wait()
        for s in range(samples):
            for condition, copy in zip(sends_across, across[s]):
                pl.when(condition)(copy.start)

    def start_rims(s):
        pl.when(gets_across)(across[s][0].wait_recv)
        for conditions, copies in ((sends_down, down[s]), (sends_up, up[s])):
            for condition, copy in zip(conditions, copies):
                pl.when(condition)(copy.start)

        @pl.when(p == 0)
        def _():
            rim_near[0, s] = jnp.zeros(rim_near.shape[2:], BF16)

        @pl.when(p == gone)
        def _():
            rim_near[1, s] = jnp.zeros(rim_near.shape[2:], BF16)

    near_queries(0)
    near_keys(0)
    near_queries(1)
    start_rims_across()
    wait_far_queries(0)
    with jax.named_scope("attend_near"):
        attend_near(0, units)
    near_keys(1)
    far(0)
    wait_far_queries(1)
    for s, some in enumerate((units[:heads], units[heads:])):
        with jax.named_scope("attend_near"):
            attend_near(1, some)
        start_rims(s)
    relay_parts(0)
    far(1)

    with jax.named_scope("wait_loads"):
        for load in loads[6:]:
            load.wait()

    row = lax.broadcasted_iota(jnp.int32, (tokens, chans), 0)

    def merge_columns(left, mid, right):
        lefts = jnp.where(row == 0, 0.0, pltpu.roll(left, 1, 0))
        rights = jnp.where(row == tokens - 1, 0.0, pltpu.roll(right, tokens - 1, 0))
        return lefts + mid + rights

    def finish(s):
        with jax.named_scope("wait_parts"):
            for copy in plain[s] + merged[s][0] + merged[s][1]:
                copy.wait_recv()
        with jax.named_scope("merge"):
            levels = [lse[s, 0], lse_in[s, 0], lse_in[s, 1]]
            top = functools.reduce(jnp.maximum, levels)
            scaled = [jnp.exp(level - top) for level in levels]
            inverse = 1.0 / functools.reduce(jnp.add, scaled)
            shares = [e * inverse for e in scaled]
            for j in range(pairs):
                totals = []
                for h in (2 * j, 2 * j + 1):
                    rows = slice(h * HEAD_DIM, (h + 1) * HEAD_DIM)
                    total = shares[0][h : h + 1] * part[s, 0, rows].astype(F32)
                    for b in range(2):
                        total = total + shares[b + 1][h : h + 1] * part_in[s, b, rows].astype(F32)
                    totals.append(total)
                att[s, :, j * 128 : (j + 1) * 128] = jnp.concatenate(totals, 0).T.astype(BF16)
        with jax.named_scope("out_proj"):
            for cols in blocks:
                value = hidden[s, :, cols].astype(F32) + dot(att[s], w_out[:, cols])
                value = value.astype(BF16)
                res[s, :, cols] = value
                value = value.astype(F32)
                mean = jnp.mean(value, 0, keepdims=True)
                centred = value - mean
                gst[s, 0, 0:1, cols] = mean
                gst[s, 0, 1:2, cols] = jnp.sum(centred * centred, 0, keepdims=True)
        copies = [
            remote(gst.at[s, 0], gst.at[s, k], gsend.at[s, k - 1], grecv.at[s, k - 1], peer(k))
            for k in range(1, n_patch)
        ]
        for copy in copies:
            copy.start()
        return copies

    results = [pltpu.make_async_copy(out.at[s], out_hbm.at[s], out_sem.at[s]) for s in range(samples)]

    def group_sum(values):
        high = values.astype(BF16).astype(F32)
        rest = values - high
        mid = rest.astype(BF16).astype(F32)
        tail = rest - mid
        stack = jnp.concatenate([high, mid, tail, jnp.zeros((5, chans), F32)], 0).astype(BF16)
        sums = dot(stack, proj[...])
        return sums[0:1] + sums[1:2] + sums[2:3]

    def normalise(s, copies):
        with jax.named_scope("wait_stats"):
            for copy in copies:
                copy.wait_recv()
        with jax.named_scope("stats"):
            stats = [gst[s, k] for k in range(n_patch)]
            mean = group_sum(functools.reduce(jnp.add, stats)[0:1] / n_patch) / width
            squares = jnp.zeros((1, chans), F32)
            for stat in stats:
                gap = stat[0:1] - mean
                squares = squares + (stat[1:2] + tokens * (gap * gap))
            var = group_sum(squares) / (n_patch * tokens * width)
            rate = lax.rsqrt(var + EPSILON)
        with jax.named_scope("silu"):
            for r in range(0, tokens, 32):
                value = (res[s, r : r + 32].astype(F32) - mean) * rate
                value = value * gn_gain[...].reshape(1, chans) + gn_bias[...].reshape(1, chans)
                act[s, r : r + 32] = (value / (1.0 + jnp.exp(-value))).astype(BF16)
        with jax.named_scope("conv"):
            taps = [dot(act[s], conv_w[1, b]) for b in range(3)]
            out[s] = (merge_columns(*taps) + rim_sum[s] + res[s].astype(F32)).astype(BF16)
        results[s].start()

    def rim_taps(s):
        with jax.named_scope("wait_rims"):
            pl.when(p > 0)(down[s][0].wait_recv)
            pl.when(p < gone)(up[s][0].wait_recv)
        with jax.named_scope("rim_taps"):
            taps = [dot(rim_near[0, s], conv_w[0, b]) + dot(rim_near[1, s], conv_w[2, b]) for b in range(3)]
            rim_sum[s] = merge_columns(*taps) + conv_b[...].reshape(1, chans) + shift[s : s + 1]

    stat_copies = [finish(0)]
    relay_parts(1)
    rim_taps(0)
    stat_copies.append(finish(1))
    rim_taps(1)
    normalise(0, stat_copies[0])
    normalise(1, stat_copies[1])

    for s in range(samples):
        results[s].wait()
        for copy in zc[s] + qc[s]:
            copy.wait_send()
        for copy in hops[s][0] + hops[s][1] + plain[s] + merged[s][0] + merged[s][1] + tuple(stat_copies[s]):
            copy.wait_send()
        for conditions, copies in ((sends_across, across[s]), (sends_down, down[s]), (sends_up, up[s])):
            for condition, copy in zip(conditions, copies):
                pl.when(condition)(copy.wait_send)


def shards(
    hidden,
    stale_attn_in,
    stale_conv_in,
    ln_gain,
    ln_bias,
    w_qkv,
    w_out,
    gn_gain,
    gn_bias,
    conv_weight,
    conv_bias,
    time_shift,
):
    samples, rows, tokens, chans = hidden.shape
    block = (samples, rows * tokens, chans)
    operands = (
        hidden.reshape(block),
        stale_attn_in.reshape(block),
        stale_conv_in.reshape(block),
        ln_gain,
        ln_bias,
        w_qkv,
        w_out,
        gn_gain,
        gn_bias,
        conv_weight,
        conv_bias,
        time_shift,
    )
    dma = pltpu.SemaphoreType.DMA
    vector = pltpu.VMEM((chans,), F32)
    out = pl.pallas_call(
        kernel,
        out_shape=jax.ShapeDtypeStruct(block, BF16),
        in_specs=[pl.BlockSpec(memory_space=pl.ANY)] * len(operands),
        out_specs=pl.BlockSpec(memory_space=pl.ANY),
        scratch_shapes=[
            pltpu.VMEM(block, BF16),
            pltpu.VMEM(block, BF16),
            pltpu.VMEM(block, BF16),
            pltpu.VMEM((2,) + block, BF16),
            pltpu.VMEM(block, BF16),
            vector,
            vector,
            pltpu.VMEM(w_qkv.shape, BF16),
            pltpu.VMEM(w_out.shape, BF16),
            vector,
            vector,
            pltpu.VMEM(conv_weight.shape, BF16),
            vector,
            pltpu.VMEM(time_shift.shape, F32),
            pltpu.VMEM(block, BF16),
            pltpu.VMEM((samples, SIDE, tokens, chans), BF16),
            pltpu.VMEM((samples, SIDE, tokens, chans), BF16),
            pltpu.VMEM((samples, 5 * tokens, chans), BF16),
            pltpu.VMEM((chans, chans), BF16),
            pltpu.VMEM((samples, chans // HEAD_DIM * HEAD_ROWS, 5 * tokens), BF16),
            pltpu.VMEM((4, 4 * tokens, 2 * tokens), F32),
            pltpu.VMEM((4, 4 * tokens, 2 * tokens), BF16),
            pltpu.VMEM((samples, 2, chans // HEAD_DIM * HEAD_ROWS, 2 * tokens), F32),
            pltpu.VMEM((samples, SIDE, chans, tokens), BF16),
            pltpu.VMEM((samples, 2, chans, tokens), BF16),
            pltpu.VMEM((samples, 2, chans // 2, tokens), BF16),
            pltpu.VMEM((samples, SIDE, 16, tokens), F32),
            pltpu.VMEM((samples, 2, 16, tokens), F32),
            pltpu.VMEM((samples, 2, 16, tokens), F32),
            pltpu.VMEM(block, BF16),
            pltpu.VMEM(block, BF16),
            pltpu.VMEM((samples, SIDE * SIDE, 2, chans), F32),
            pltpu.VMEM((chans, chans), BF16),
            pltpu.VMEM(block, F32),
            pltpu.VMEM(block, BF16),
            pltpu.VMEM(block, BF16),
            dma((12,)),
            dma((samples,)),
            dma((samples, 4)),
            dma((samples, 4)),
            dma((samples, 4)),
            dma((samples, 4)),
            dma((samples, 10)),
            dma((samples, 10)),
            dma((samples, 3)),
            dma((samples, 3)),
            dma((samples, SIDE * SIDE - 1)),
            dma((samples, SIDE * SIDE - 1)),
        ],
        compiler_params=pltpu.CompilerParams(
            collective_id=0, has_side_effects=True, vmem_limit_bytes=60 * 1024 * 1024
        ),
        name="section",
    )(*operands)
    return out.reshape(hidden.shape)


def solution(mesh):
    spread = P("img", "patch", None, None)
    return jax.shard_map(
        shards,
        mesh=mesh,
        in_specs=(spread, spread, spread) + (P(),) * 8 + (P("img", None),),
        out_specs=spread,
        check_vma=False,
    )
```

```python
import functools

import jax
import jax.numpy as jnp
from jax import lax
from jax.experimental import pallas as pl
from jax.experimental.pallas import tpu as pltpu
from jax.sharding import PartitionSpec as P

GROUPS = 32
HEAD_DIM = 64
HEAD_ROWS = 80
SIDE = 4
EPSILON = 1e-05
MESH = pl.DeviceIdType.MESH
F32 = jnp.float32
BF16 = jnp.bfloat16


def dot_nt(a, b):
    return lax.dot_general(a, b, (((1,), (1,)), ((), ())), preferred_element_type=F32)


def dot(a, b):
    return jnp.dot(a, b, preferred_element_type=F32)


def kernel(
    hidden_hbm,
    stale_hbm,
    rim_hbm,
    ln_gain_hbm,
    ln_bias_hbm,
    w_qkv_hbm,
    w_out_hbm,
    gn_gain_hbm,
    gn_bias_hbm,
    conv_w_hbm,
    conv_b_hbm,
    shift_hbm,
    out,
    hidden,
    stale,
    rim_own,
    rim_near,
    rim_hop,
    ln_gain,
    ln_bias,
    w_qkv,
    w_out,
    gn_gain,
    gn_bias,
    conv_w,
    conv_b,
    shift,
    fresh,
    zbuf,
    qbuf,
    kbuf,
    w_vt,
    vt,
    scores,
    weights,
    sums,
    part,
    part_in,
    hop,
    lse,
    lse_in,
    lse_hop,
    att,
    res,
    gst,
    proj,
    rim_sum,
    act,
    load_sem,
    zsend,
    zrecv,
    qsend,
    qrecv,
    osend,
    orecv,
    rsend,
    rrecv,
    gsend,
    grecv,
):
    n_patch = SIDE * SIDE
    samples, tokens, chans = hidden.shape
    half = tokens // 2
    p = lax.axis_index("patch")
    y, z = p // SIDE, p % SIDE
    z_next = {"patch": y * SIDE + (z + 1) % SIDE}
    z_prev = {"patch": y * SIDE + (z + SIDE - 1) % SIDE}
    y_next = {"patch": ((y + 1) % SIDE) * SIDE + z}
    y_prev = {"patch": ((y + SIDE - 1) % SIDE) * SIDE + z}

    def peer(k):
        return {"patch": (p + k) % n_patch}

    loads = []
    for i, (src, dst) in enumerate(
        (
            (stale_hbm, stale),
            (ln_gain_hbm, ln_gain),
            (ln_bias_hbm, ln_bias),
            (hidden_hbm, hidden),
            (w_qkv_hbm, w_qkv),
            (rim_hbm, rim_own),
            (w_out_hbm, w_out),
            (gn_gain_hbm, gn_gain),
            (gn_bias_hbm, gn_bias),
            (conv_b_hbm, conv_b),
            (shift_hbm, shift),
            (conv_w_hbm, conv_w),
        )
    ):
        load = pltpu.make_async_copy(src, dst, load_sem.at[i])
        load.start()
        loads.append(load)

    barrier = pltpu.get_barrier_semaphore()
    for target in (z_next, z_prev, y_next, y_prev):
        pl.semaphore_signal(barrier, inc=1, device_id=target, device_id_type=MESH)

    def remote(src, dst, send, recv, target):
        return pltpu.make_async_remote_copy(
            src_ref=src, dst_ref=dst, send_sem=send, recv_sem=recv, device_id=target, device_id_type=MESH
        )

    def ring(buf, send, recv, s, nxt, prv):
        return (
            remote(buf.at[s, 0], buf.at[s, 1], send.at[s, 0], recv.at[s, 0], nxt),
            remote(buf.at[s, 0], buf.at[s, 2], send.at[s, 1], recv.at[s, 1], prv),
            remote(
                buf.at[s, 1, pl.ds(0, half)], buf.at[s, 3, pl.ds(0, half)], send.at[s, 2], recv.at[s, 2], nxt
            ),
            remote(
                buf.at[s, 2, pl.ds(half, half)],
                buf.at[s, 3, pl.ds(half, half)],
                send.at[s, 3],
                recv.at[s, 3],
                prv,
            ),
        )

    zc = [ring(zbuf, zsend, zrecv, s, z_next, z_prev) for s in range(samples)]
    qc = [ring(qbuf, qsend, qrecv, s, y_next, y_prev) for s in range(samples)]

    def layer_norm(values):
        values = values.astype(F32)
        centre = jnp.mean(values, -1, keepdims=True)
        centred = values - centre
        spread = jnp.mean(centred * centred, -1, keepdims=True)
        return (centred * lax.rsqrt(spread + EPSILON) * ln_gain[...].reshape(1, chans) + ln_bias[...].reshape(1, chans)).astype(BF16)

    step = 32
    blocks = [slice(c, min(c + 256, chans)) for c in range(0, chans, 256)]
    def norm_stale(s):
        with jax.named_scope("norm_stale"):

            @pl.loop(0, tokens // step, unroll=True)
            def _(i):
                rows = pl.ds(pl.multiple_of(i * step, step), step)
                zbuf[s, 0, rows] = layer_norm(stale[s, rows])

    for load in loads[:3]:
        load.wait()
    norm_stale(0)
    with jax.named_scope("barrier"):
        pl.semaphore_wait(barrier, 4)
    for s in range(samples):
        if s > 0:
            norm_stale(s)
        zc[s][0].start()
        zc[s][1].start()

    with jax.named_scope("norm_fresh"):
        loads[3].wait()
        for s in range(samples):

            @pl.loop(0, tokens // step, unroll=True)
            def _(i):
                rows = pl.ds(pl.multiple_of(i * step, step), step)
                fresh[s, rows] = layer_norm(hidden[s, rows])

    with jax.named_scope("turn_weights"):
        lse[...] = jnp.zeros(lse.shape, F32)
        loads[4].wait()
        for r in range(0, chans, 128):
            for c in range(0, chans, 128):
                block = w_qkv[r : r + 128, 2 * chans + c : 2 * chans + c + 128]
                w_vt[c : c + 128, r : r + 128] = block.astype(F32).T.astype(BF16)
        for u in range(2):
            weights[2 * u, 3 * tokens :, :tokens] = jnp.zeros((tokens, tokens), BF16)
            weights[2 * u, :tokens, tokens:] = jnp.zeros((tokens, tokens), BF16)

    with jax.named_scope("queries"):
        for s in range(samples):
            for cols in blocks:
                q = dot(fresh[s], w_qkv[:, cols]).astype(BF16)
                qbuf[s, 0, :, cols] = q * BF16(HEAD_DIM**-0.5)
            qc[s][0].start()
            qc[s][1].start()

    heads = chans // HEAD_DIM

    def project(src, s, block, count):
        rows = slice(block * tokens, (block + count) * tokens)
        for cols in blocks:
            kbuf[s, rows, cols] = dot(src, w_qkv[:, chans + cols.start : chans + cols.stop]).astype(BF16)
        values = dot_nt(w_vt[...], src).astype(BF16)
        for h in range(heads):
            vt[s, h * HEAD_ROWS : h * HEAD_ROWS + HEAD_DIM, rows] = values[h * HEAD_DIM : (h + 1) * HEAD_DIM]

    with jax.named_scope("own_pairs"):
        for s in range(samples):
            project(fresh[s], s, 0, 1)
            project(zbuf[s, 0], s, 3, 1)
            for h in range(heads):
                vt[s, h * HEAD_ROWS + HEAD_DIM : (h + 1) * HEAD_ROWS, :] = jnp.ones(
                    (HEAD_ROWS - HEAD_DIM, 5 * tokens), BF16
                )

    width = chans // GROUPS

    def group_of(v):
        return (v * (65536 // width + 1)) >> 16

    for r in range(0, chans, 128):
        same = group_of(lax.broadcasted_iota(jnp.int32, (128, chans), 0) + r) == group_of(
            lax.broadcasted_iota(jnp.int32, (128, chans), 1)
        )
        proj[r : r + 128] = jnp.where(same, 1.0, 0.0).astype(BF16)

    keys = 3 * tokens
    pairs = chans // 128
    low = lax.broadcasted_iota(jnp.int32, (2 * tokens, 128), 1) < HEAD_DIM
    units = [(head, t) for head in range(heads) for t in range(2)]

    def masked_queries(s, head, t):
        cols = slice(head // 2 * 128, head // 2 * 128 + 128)
        queries = qbuf[s, 2 * t : 2 * t + 2, :, cols].reshape(2 * tokens, 128)
        return cols, jnp.where(low if head % 2 == 0 else ~low, queries, BF16(0))

    def attend_near(s, units):
        peaks = {}

        def score(i):
            head, t = units[i]
            u = i % 4
            first = 0 if t == 0 else tokens
            cols, queries = masked_queries(s, head, t)
            value = dot_nt(kbuf[s, first : 4 * tokens, cols], queries)
            if t == 0:
                scores[u] = value
                peaks[i] = (
                    jnp.max(value[:keys, :tokens], 0, keepdims=True),
                    jnp.max(value[tokens:, tokens:], 0, keepdims=True),
                )
            else:
                scores[u, tokens:] = value
                top = jnp.max(value, 0, keepdims=True)
                peaks[i] = (top[:, :tokens], top[:, tokens:])

        def apply(i):
            head, t = units[i]
            u = i % 4
            for half, top in enumerate(peaks[i]):
                lanes = slice(half * tokens, (half + 1) * tokens)
                first = 0 if t == 0 and half == 0 else tokens
                rows = slice(first, first + keys)
                weights[u, rows, lanes] = jnp.exp(scores[u, rows, lanes] - top).astype(BF16)
            mine = slice(head * HEAD_ROWS, (head + 1) * HEAD_ROWS)
            first = 0 if t == 0 else tokens
            sums[s, t, mine] = dot(vt[s, mine, first : 4 * tokens], weights[u, first:])
            spare = slice(head * HEAD_ROWS + HEAD_DIM + 8, (head + 1) * HEAD_ROWS)
            sums[s, t, spare] = jnp.broadcast_to(jnp.concatenate(peaks[i], 1), (8, 2 * tokens))

        ahead = 3
        for i in range(len(units) + ahead):
            if i < len(units):
                score(i)
            if i >= ahead:
                apply(i - ahead)

    def attend_far(s, mine):
        values, gains = {}, {}

        def score(i):
            head, t = mine[i]
            cols, queries = masked_queries(s, head, t)
            values[i] = dot_nt(kbuf[s, 4 * tokens :, cols], queries)

        def weigh(i):
            head, t = mine[i]
            spare = slice(head * HEAD_ROWS + HEAD_DIM + 8, (head + 1) * HEAD_ROWS)
            before = sums[s, t, spare][0:1]
            top = jnp.maximum(before, jnp.max(values[i], 0, keepdims=True))
            gains[i] = (jnp.exp(before - top), top)
            values[i] = jnp.exp(values[i] - top).astype(BF16)

        def apply(i):
            head, t = mine[i]
            gain, top = gains[i]
            rows = slice(head * HEAD_ROWS, (head + 1) * HEAD_ROWS)
            total = sums[s, t, rows] * gain + dot(vt[s, rows, 4 * tokens :], values[i])
            norm = total[HEAD_DIM : HEAD_DIM + 1]
            ratio = (total[:HEAD_DIM] * (1.0 / norm)).astype(BF16)
            level = top + jnp.log(norm)
            for half in range(2):
                lanes = slice(half * tokens, (half + 1) * tokens)
                b = 2 * t + half
                part[s, b, head * HEAD_DIM : (head + 1) * HEAD_DIM] = ratio[:, lanes]
                lse[s, b, head : head + 1] = level[:, lanes]

        for i in range(len(mine) + 2):
            if i < len(mine):
                score(i)
            if 0 <= i - 1 < len(mine):
                weigh(i - 1)
            if 0 <= i - 2 < len(mine):
                apply(i - 2)

    upper, lower = pl.ds(0, chans // 2), pl.ds(chans // 2, chans // 2)
    hops, plain, merged = [], [], []
    for s in range(samples):

        def to(i, src, dst, target):
            return remote(src, dst, osend.at[s, i], orecv.at[s, i], target)

        hops.append(
            (
                (to(0, part.at[s, 3, upper], hop.at[s, 0], y_next), to(2, lse.at[s, 3], lse_hop.at[s, 0], y_next)),
                (to(1, part.at[s, 3, lower], hop.at[s, 1], y_prev), to(3, lse.at[s, 3], lse_hop.at[s, 1], y_prev)),
            )
        )
        plain.append(
            (
                to(4, part.at[s, 1, upper], part_in.at[s, 1, upper], y_prev),
                to(5, part.at[s, 2, lower], part_in.at[s, 0, lower], y_next),
            )
        )
        merged.append(
            (
                (to(6, part.at[s, 2, upper], part_in.at[s, 0, upper], y_next), to(8, lse.at[s, 2], lse_in.at[s, 0], y_next)),
                (to(7, part.at[s, 1, lower], part_in.at[s, 1, lower], y_prev), to(9, lse.at[s, 1], lse_in.at[s, 1], y_prev)),
            )
        )

    def send_parts(s, n):
        if n < 2:
            hops[s][n][0].start()
        if n == 1:
            hops[s][0][1].start()
            hops[s][1][1].start()
            plain[s][1].start()
        if n == 2:
            plain[s][0].start()

    def relay_parts(s):
        for n, b in ((0, 2), (1, 1)):
            with jax.named_scope("wait_hops"):
                for copy in hops[s][n]:
                    copy.wait_recv()
            with jax.named_scope("add_hops"):
                near_level, far_level = lse[s, b], lse_hop[s, n]
                top = jnp.maximum(near_level, far_level)
                near_scale, far_scale = jnp.exp(near_level - top), jnp.exp(far_level - top)
                total = near_scale + far_scale
                near_scale, far_scale = near_scale / total, far_scale / total
                first = n * heads // 2
                for h in range(first, first + heads // 2):
                    rows = slice(h * HEAD_DIM, (h + 1) * HEAD_DIM)
                    there = slice((h - first) * HEAD_DIM, (h - first + 1) * HEAD_DIM)
                    value = near_scale[h : h + 1] * part[s, b, rows].astype(F32)
                    value = value + far_scale[h : h + 1] * hop[s, n, there].astype(F32)
                    part[s, b, rows] = value.astype(BF16)
                lse[s, b, first : first + heads // 2] = (top + jnp.log(total))[first : first + heads // 2]
            for copy in merged[s][n]:
                copy.start()

    def near_queries(s):
        with jax.named_scope("wait_q_near"):
            qc[s][0].wait_recv()
            qc[s][2].start()
            qc[s][1].wait_recv()
            qc[s][3].start()

    def near_keys(s):
        with jax.named_scope("wait_z_near"):
            zc[s][0].wait_recv()
            zc[s][2].start()
            zc[s][1].wait_recv()
            zc[s][3].start()
        with jax.named_scope("near_pairs"):
            project(zbuf[s, 1:3].reshape(2 * tokens, chans), s, 1, 2)

    def far(s):
        with jax.named_scope("wait_z_far"):
            zc[s][2].wait_recv()
            zc[s][3].wait_recv()
        with jax.named_scope("far_pairs"):
            project(zbuf[s, 3], s, 4, 1)
        first, second = range(heads // 2), range(heads // 2, heads)
        for n, mine in enumerate(([(h, 1) for h in first], [(h, 1) for h in second], [(h, 0) for h in range(heads)])):
            with jax.named_scope("attend_far"):
                attend_far(s, mine)
            send_parts(s, n)

    def wait_far_queries(s):
        with jax.named_scope("wait_q_far"):
            qc[s][2].wait_recv()
            qc[s][3].wait_recv()

    last, gone = SIDE - 1, n_patch - 1
    sends_across = (jnp.logical_and(z == last, y < last), jnp.logical_and(z == 0, y > 0))
    gets_across = jnp.logical_or(jnp.logical_and(z == last, y > 0), jnp.logical_and(z == 0, y < last))
    sends_down = (z < last, jnp.logical_and(z == last, y > 0))
    sends_up = (z > 0, jnp.logical_and(z == 0, y < last))
    across, down, up = [], [], []
    for s in range(samples):

        def rim(i, src, dst, target):
            return remote(src.at[s], dst.at[s], rsend.at[s, i], rrecv.at[s, i], target)

        across.append([rim(2, rim_own, rim_hop, target) for target in (y_next, y_prev)])
        down.append([rim(0, src, rim_near.at[0], z_next) for src in (rim_own, rim_hop)])
        up.append([rim(1, src, rim_near.at[1], z_prev) for src in (rim_own, rim_hop)])

    def start_rims_across():
        loads[5].wait()
        for s in range(samples):
            for condition, copy in zip(sends_across, across[s]):
                pl.when(condition)(copy.start)

    def start_rims(s):
        pl.when(gets_across)(across[s][0].wait_recv)
        for conditions, copies in ((sends_down, down[s]), (sends_up, up[s])):
            for condition, copy in zip(conditions, copies):
                pl.when(condition)(copy.start)

        @pl.when(p == 0)
        def _():
            rim_near[0, s] = jnp.zeros(rim_near.shape[2:], BF16)

        @pl.when(p == gone)
        def _():
            rim_near[1, s] = jnp.zeros(rim_near.shape[2:], BF16)

    near_queries(0)
    near_keys(0)
    near_queries(1)
    start_rims_across()
    wait_far_queries(0)
    with jax.named_scope("attend_near"):
        attend_near(0, units)
    near_keys(1)
    far(0)
    start_rims(0)
    wait_far_queries(1)
    with jax.named_scope("attend_near"):
        attend_near(1, units)
    relay_parts(0)
    start_rims(1)
    far(1)

    with jax.named_scope("wait_loads"):
        for load in loads[6:]:
            load.wait()

    row = lax.broadcasted_iota(jnp.int32, (tokens, chans), 0)

    def merge_columns(left, mid, right):
        lefts = jnp.where(row == 0, 0.0, pltpu.roll(left, 1, 0))
        rights = jnp.where(row == tokens - 1, 0.0, pltpu.roll(right, tokens - 1, 0))
        return lefts + mid + rights

    def finish(s):
        with jax.named_scope("wait_parts"):
            for copy in plain[s] + merged[s][0] + merged[s][1]:
                copy.wait_recv()
        with jax.named_scope("merge"):
            levels = [lse[s, 0], lse_in[s, 0], lse_in[s, 1]]
            top = functools.reduce(jnp.maximum, levels)
            scaled = [jnp.exp(level - top) for level in levels]
            inverse = 1.0 / functools.reduce(jnp.add, scaled)
            shares = [e * inverse for e in scaled]
            for j in range(pairs):
                totals = []
                for h in (2 * j, 2 * j + 1):
                    rows = slice(h * HEAD_DIM, (h + 1) * HEAD_DIM)
                    total = shares[0][h : h + 1] * part[s, 0, rows].astype(F32)
                    for b in range(2):
                        total = total + shares[b + 1][h : h + 1] * part_in[s, b, rows].astype(F32)
                    totals.append(total)
                att[s, :, j * 128 : (j + 1) * 128] = jnp.concatenate(totals, 0).T.astype(BF16)
        with jax.named_scope("out_proj"):
            for cols in blocks:
                value = hidden[s, :, cols].astype(F32) + dot(att[s], w_out[:, cols])
                value = value.astype(BF16)
                res[s, :, cols] = value
                value = value.astype(F32)
                mean = jnp.mean(value, 0, keepdims=True)
                centred = value - mean
                gst[s, 0, 0:1, cols] = mean
                gst[s, 0, 1:2, cols] = jnp.sum(centred * centred, 0, keepdims=True)
        copies = [
            remote(gst.at[s, 0], gst.at[s, k], gsend.at[s, k - 1], grecv.at[s, k - 1], peer(k))
            for k in range(1, n_patch)
        ]
        for copy in copies:
            copy.start()
        return copies

    def group_sum(values):
        high = values.astype(BF16).astype(F32)
        rest = values - high
        mid = rest.astype(BF16).astype(F32)
        tail = rest - mid
        stack = jnp.concatenate([high, mid, tail, jnp.zeros((5, chans), F32)], 0).astype(BF16)
        sums = dot(stack, proj[...])
        return sums[0:1] + sums[1:2] + sums[2:3]

    def normalise(s, copies):
        with jax.named_scope("wait_stats"):
            for copy in copies:
                copy.wait_recv()
        with jax.named_scope("stats"):
            stats = [gst[s, k] for k in range(n_patch)]
            mean = group_sum(functools.reduce(jnp.add, stats)[0:1] / n_patch) / width
            squares = jnp.zeros((1, chans), F32)
            for stat in stats:
                gap = stat[0:1] - mean
                squares = squares + (stat[1:2] + tokens * (gap * gap))
            var = group_sum(squares) / (n_patch * tokens * width)
            rate = lax.rsqrt(var + EPSILON)
        with jax.named_scope("silu"):
            for r in range(0, tokens, 32):
                value = (res[s, r : r + 32].astype(F32) - mean) * rate
                value = value * gn_gain[...].reshape(1, chans) + gn_bias[...].reshape(1, chans)
                act[s, r : r + 32] = (value / (1.0 + jnp.exp(-value))).astype(BF16)
        with jax.named_scope("conv"):
            taps = [dot(act[s], conv_w[1, b]) for b in range(3)]
            out[s] = (merge_columns(*taps) + rim_sum[s] + res[s].astype(F32)).astype(BF16)

    def rim_taps(s):
        with jax.named_scope("wait_rims"):
            pl.when(p > 0)(down[s][0].wait_recv)
            pl.when(p < gone)(up[s][0].wait_recv)
        with jax.named_scope("rim_taps"):
            taps = [dot(rim_near[0, s], conv_w[0, b]) + dot(rim_near[1, s], conv_w[2, b]) for b in range(3)]
            rim_sum[s] = merge_columns(*taps) + conv_b[...].reshape(1, chans) + shift[s : s + 1]

    stat_copies = [finish(0)]
    relay_parts(1)
    stat_copies.append(finish(1))
    rim_taps(0)
    rim_taps(1)
    normalise(0, stat_copies[0])
    normalise(1, stat_copies[1])

    for s in range(samples):
        for copy in zc[s] + qc[s]:
            copy.wait_send()
        for copy in hops[s][0] + hops[s][1] + plain[s] + merged[s][0] + merged[s][1] + tuple(stat_copies[s]):
            copy.wait_send()
        for conditions, copies in ((sends_across, across[s]), (sends_down, down[s]), (sends_up, up[s])):
            for condition, copy in zip(conditions, copies):
                pl.when(condition)(copy.wait_send)


def shards(
    hidden,
    stale_attn_in,
    stale_conv_in,
    ln_gain,
    ln_bias,
    w_qkv,
    w_out,
    gn_gain,
    gn_bias,
    conv_weight,
    conv_bias,
    time_shift,
):
    samples, rows, tokens, chans = hidden.shape
    block = (samples, rows * tokens, chans)
    operands = (
        hidden.reshape(block),
        stale_attn_in.reshape(block),
        stale_conv_in.reshape(block),
        ln_gain,
        ln_bias,
        w_qkv,
        w_out,
        gn_gain,
        gn_bias,
        conv_weight,
        conv_bias,
        time_shift,
    )
    dma = pltpu.SemaphoreType.DMA
    vector = pltpu.VMEM((chans,), F32)
    out = pl.pallas_call(
        kernel,
        out_shape=jax.ShapeDtypeStruct(block, BF16),
        in_specs=[pl.BlockSpec(memory_space=pl.ANY)] * len(operands),
        out_specs=pl.BlockSpec(memory_space=pltpu.VMEM),
        scratch_shapes=[
            pltpu.VMEM(block, BF16),
            pltpu.VMEM(block, BF16),
            pltpu.VMEM(block, BF16),
            pltpu.VMEM((2,) + block, BF16),
            pltpu.VMEM(block, BF16),
            vector,
            vector,
            pltpu.VMEM(w_qkv.shape, BF16),
            pltpu.VMEM(w_out.shape, BF16),
            vector,
            vector,
            pltpu.VMEM(conv_weight.shape, BF16),
            vector,
            pltpu.VMEM(time_shift.shape, F32),
            pltpu.VMEM(block, BF16),
            pltpu.VMEM((samples, SIDE, tokens, chans), BF16),
            pltpu.VMEM((samples, SIDE, tokens, chans), BF16),
            pltpu.VMEM((samples, 5 * tokens, chans), BF16),
            pltpu.VMEM((chans, chans), BF16),
            pltpu.VMEM((samples, chans // HEAD_DIM * HEAD_ROWS, 5 * tokens), BF16),
            pltpu.VMEM((4, 4 * tokens, 2 * tokens), F32),
            pltpu.VMEM((4, 4 * tokens, 2 * tokens), BF16),
            pltpu.VMEM((samples, 2, chans // HEAD_DIM * HEAD_ROWS, 2 * tokens), F32),
            pltpu.VMEM((samples, SIDE, chans, tokens), BF16),
            pltpu.VMEM((samples, 2, chans, tokens), BF16),
            pltpu.VMEM((samples, 2, chans // 2, tokens), BF16),
            pltpu.VMEM((samples, SIDE, 16, tokens), F32),
            pltpu.VMEM((samples, 2, 16, tokens), F32),
            pltpu.VMEM((samples, 2, 16, tokens), F32),
            pltpu.VMEM(block, BF16),
            pltpu.VMEM(block, BF16),
            pltpu.VMEM((samples, SIDE * SIDE, 2, chans), F32),
            pltpu.VMEM((chans, chans), BF16),
            pltpu.VMEM(block, F32),
            pltpu.VMEM(block, BF16),
            dma((12,)),
            dma((samples, 4)),
            dma((samples, 4)),
            dma((samples, 4)),
            dma((samples, 4)),
            dma((samples, 10)),
            dma((samples, 10)),
            dma((samples, 3)),
            dma((samples, 3)),
            dma((samples, SIDE * SIDE - 1)),
            dma((samples, SIDE * SIDE - 1)),
        ],
        compiler_params=pltpu.CompilerParams(
            collective_id=0, has_side_effects=True, vmem_limit_bytes=42 * 1024 * 1024
        ),
        name="section",
    )(*[pltpu.with_memory_space_constraint(x, pltpu.HBM) for x in operands])
    return out.reshape(hidden.shape)


def solution(mesh):
    spread = P("img", "patch", None, None)
    return jax.shard_map(
        shards,
        mesh=mesh,
        in_specs=(spread, spread, spread) + (P(),) * 8 + (P("img", None),),
        out_specs=spread,
        check_vma=False,
    )
```

```python
import functools

import jax
import jax.numpy as jnp
from jax import lax
from jax.experimental import pallas as pl
from jax.experimental.pallas import tpu as pltpu
from jax.sharding import PartitionSpec as P

GROUPS = 32
HEAD_DIM = 64
HEAD_ROWS = 80
SIDE = 4
EPSILON = 1e-05
MESH = pl.DeviceIdType.MESH
F32 = jnp.float32
BF16 = jnp.bfloat16


def dot_nt(a, b):
    return lax.dot_general(a, b, (((1,), (1,)), ((), ())), preferred_element_type=F32)


def dot(a, b):
    return jnp.dot(a, b, preferred_element_type=F32)


def kernel(
    hidden_hbm,
    stale_hbm,
    rim_hbm,
    ln_gain_hbm,
    ln_bias_hbm,
    w_qkv_hbm,
    w_out_hbm,
    gn_gain_hbm,
    gn_bias_hbm,
    conv_w_hbm,
    conv_b_hbm,
    shift_hbm,
    out,
    hidden,
    stale,
    rim_own,
    rim_near,
    rim_hop,
    ln_gain,
    ln_bias,
    w_qkv,
    w_out,
    gn_gain,
    gn_bias,
    conv_w,
    conv_b,
    shift,
    fresh,
    zbuf,
    qbuf,
    kbuf,
    w_vt,
    vt,
    scores,
    weights,
    sums,
    part,
    part_in,
    hop,
    lse,
    lse_in,
    lse_hop,
    att,
    res,
    gst,
    proj,
    rim_sum,
    act,
    load_sem,
    zsend,
    zrecv,
    qsend,
    qrecv,
    osend,
    orecv,
    rsend,
    rrecv,
    gsend,
    grecv,
):
    n_patch = SIDE * SIDE
    samples, tokens, chans = hidden.shape
    half = tokens // 2
    p = lax.axis_index("patch")
    y, z = p // SIDE, p % SIDE
    z_next = {"patch": y * SIDE + (z + 1) % SIDE}
    z_prev = {"patch": y * SIDE + (z + SIDE - 1) % SIDE}
    y_next = {"patch": ((y + 1) % SIDE) * SIDE + z}
    y_prev = {"patch": ((y + SIDE - 1) % SIDE) * SIDE + z}

    def peer(k):
        return {"patch": (p + k) % n_patch}

    loads = []
    for i, (src, dst) in enumerate(
        (
            (stale_hbm, stale),
            (ln_gain_hbm, ln_gain),
            (ln_bias_hbm, ln_bias),
            (hidden_hbm, hidden),
            (w_qkv_hbm, w_qkv),
            (rim_hbm, rim_own),
            (w_out_hbm, w_out),
            (gn_gain_hbm, gn_gain),
            (gn_bias_hbm, gn_bias),
            (conv_b_hbm, conv_b),
            (shift_hbm, shift),
            (conv_w_hbm, conv_w),
        )
    ):
        load = pltpu.make_async_copy(src, dst, load_sem.at[i])
        load.start()
        loads.append(load)

    barrier = pltpu.get_barrier_semaphore()
    for target in (z_next, z_prev, y_next, y_prev):
        pl.semaphore_signal(barrier, inc=1, device_id=target, device_id_type=MESH)

    def remote(src, dst, send, recv, target):
        return pltpu.make_async_remote_copy(
            src_ref=src, dst_ref=dst, send_sem=send, recv_sem=recv, device_id=target, device_id_type=MESH
        )

    def ring(buf, send, recv, s, nxt, prv):
        return (
            remote(buf.at[s, 0], buf.at[s, 1], send.at[s, 0], recv.at[s, 0], nxt),
            remote(buf.at[s, 0], buf.at[s, 2], send.at[s, 1], recv.at[s, 1], prv),
            remote(
                buf.at[s, 1, pl.ds(0, half)], buf.at[s, 3, pl.ds(0, half)], send.at[s, 2], recv.at[s, 2], nxt
            ),
            remote(
                buf.at[s, 2, pl.ds(half, half)],
                buf.at[s, 3, pl.ds(half, half)],
                send.at[s, 3],
                recv.at[s, 3],
                prv,
            ),
        )

    zc = [ring(zbuf, zsend, zrecv, s, z_next, z_prev) for s in range(samples)]
    qc = [ring(qbuf, qsend, qrecv, s, y_next, y_prev) for s in range(samples)]

    def layer_norm(values):
        values = values.astype(F32)
        centre = jnp.mean(values, -1, keepdims=True)
        centred = values - centre
        spread = jnp.mean(centred * centred, -1, keepdims=True)
        return (centred * lax.rsqrt(spread + EPSILON) * ln_gain[...].reshape(1, chans) + ln_bias[...].reshape(1, chans)).astype(BF16)

    step = 32
    blocks = [slice(c, min(c + 256, chans)) for c in range(0, chans, 256)]
    def norm_stale(s):
        with jax.named_scope("norm_stale"):

            @pl.loop(0, tokens // step, unroll=True)
            def _(i):
                rows = pl.ds(pl.multiple_of(i * step, step), step)
                zbuf[s, 0, rows] = layer_norm(stale[s, rows])

    for load in loads[:3]:
        load.wait()
    norm_stale(0)
    with jax.named_scope("barrier"):
        pl.semaphore_wait(barrier, 4)
    for s in range(samples):
        if s > 0:
            norm_stale(s)
        zc[s][0].start()
        zc[s][1].start()

    with jax.named_scope("norm_fresh"):
        loads[3].wait()
        for s in range(samples):

            @pl.loop(0, tokens // step, unroll=True)
            def _(i):
                rows = pl.ds(pl.multiple_of(i * step, step), step)
                fresh[s, rows] = layer_norm(hidden[s, rows])

    with jax.named_scope("turn_weights"):
        lse[...] = jnp.zeros(lse.shape, F32)
        loads[4].wait()
        for r in range(0, chans, 128):
            for c in range(0, chans, 128):
                block = w_qkv[r : r + 128, 2 * chans + c : 2 * chans + c + 128]
                w_vt[c : c + 128, r : r + 128] = block.astype(F32).T.astype(BF16)
        for u in range(2):
            weights[2 * u, 3 * tokens :, :tokens] = jnp.zeros((tokens, tokens), BF16)
            weights[2 * u, :tokens, tokens:] = jnp.zeros((tokens, tokens), BF16)

    with jax.named_scope("queries"):
        for s in range(samples):
            for cols in blocks:
                q = dot(fresh[s], w_qkv[:, cols]).astype(BF16)
                qbuf[s, 0, :, cols] = q * BF16(HEAD_DIM**-0.5)
            qc[s][0].start()
            qc[s][1].start()

    heads = chans // HEAD_DIM

    def project(src, s, block, count):
        rows = slice(block * tokens, (block + count) * tokens)
        for cols in blocks:
            kbuf[s, rows, cols] = dot(src, w_qkv[:, chans + cols.start : chans + cols.stop]).astype(BF16)
        values = dot_nt(w_vt[...], src).astype(BF16)
        for h in range(heads):
            vt[s, h * HEAD_ROWS : h * HEAD_ROWS + HEAD_DIM, rows] = values[h * HEAD_DIM : (h + 1) * HEAD_DIM]

    with jax.named_scope("own_pairs"):
        for s in range(samples):
            project(fresh[s], s, 0, 1)
            project(zbuf[s, 0], s, 3, 1)
            for h in range(heads):
                vt[s, h * HEAD_ROWS + HEAD_DIM : (h + 1) * HEAD_ROWS, :] = jnp.ones(
                    (HEAD_ROWS - HEAD_DIM, 5 * tokens), BF16
                )

    width = chans // GROUPS

    def group_of(v):
        return (v * (65536 // width + 1)) >> 16

    for r in range(0, chans, 128):
        same = group_of(lax.broadcasted_iota(jnp.int32, (128, chans), 0) + r) == group_of(
            lax.broadcasted_iota(jnp.int32, (128, chans), 1)
        )
        proj[r : r + 128] = jnp.where(same, 1.0, 0.0).astype(BF16)

    keys = 3 * tokens
    pairs = chans // 128
    low = lax.broadcasted_iota(jnp.int32, (2 * tokens, 128), 1) < HEAD_DIM
    units = [(head, t) for head in range(heads) for t in range(2)]

    def masked_queries(s, head, t):
        cols = slice(head // 2 * 128, head // 2 * 128 + 128)
        queries = qbuf[s, 2 * t : 2 * t + 2, :, cols].reshape(2 * tokens, 128)
        return cols, jnp.where(low if head % 2 == 0 else ~low, queries, BF16(0))

    def attend_near(s, units):
        peaks = {}

        def score(i):
            head, t = units[i]
            u = i % 4
            first = 0 if t == 0 else tokens
            cols, queries = masked_queries(s, head, t)
            value = dot_nt(kbuf[s, first : 4 * tokens, cols], queries)
            if t == 0:
                scores[u] = value
                peaks[i] = (
                    jnp.max(value[:keys, :tokens], 0, keepdims=True),
                    jnp.max(value[tokens:, tokens:], 0, keepdims=True),
                )
            else:
                scores[u, tokens:] = value
                top = jnp.max(value, 0, keepdims=True)
                peaks[i] = (top[:, :tokens], top[:, tokens:])

        def apply(i):
            head, t = units[i]
            u = i % 4
            for half, top in enumerate(peaks[i]):
                lanes = slice(half * tokens, (half + 1) * tokens)
                first = 0 if t == 0 and half == 0 else tokens
                rows = slice(first, first + keys)
                weights[u, rows, lanes] = jnp.exp(scores[u, rows, lanes] - top).astype(BF16)
            mine = slice(head * HEAD_ROWS, (head + 1) * HEAD_ROWS)
            first = 0 if t == 0 else tokens
            sums[s, t, mine] = dot(vt[s, mine, first : 4 * tokens], weights[u, first:])
            spare = slice(head * HEAD_ROWS + HEAD_DIM + 8, (head + 1) * HEAD_ROWS)
            sums[s, t, spare] = jnp.broadcast_to(jnp.concatenate(peaks[i], 1), (8, 2 * tokens))

        ahead = 3
        for i in range(len(units) + ahead):
            if i < len(units):
                score(i)
            if i >= ahead:
                apply(i - ahead)

    def attend_far(s, mine):
        values, gains = {}, {}

        def score(i):
            head, t = mine[i]
            cols, queries = masked_queries(s, head, t)
            values[i] = dot_nt(kbuf[s, 4 * tokens :, cols], queries)

        def weigh(i):
            head, t = mine[i]
            spare = slice(head * HEAD_ROWS + HEAD_DIM + 8, (head + 1) * HEAD_ROWS)
            before = sums[s, t, spare][0:1]
            top = jnp.maximum(before, jnp.max(values[i], 0, keepdims=True))
            gains[i] = (jnp.exp(before - top), top)
            values[i] = jnp.exp(values[i] - top).astype(BF16)

        def apply(i):
            head, t = mine[i]
            gain, top = gains[i]
            rows = slice(head * HEAD_ROWS, (head + 1) * HEAD_ROWS)
            total = sums[s, t, rows] * gain + dot(vt[s, rows, 4 * tokens :], values[i])
            norm = total[HEAD_DIM : HEAD_DIM + 1]
            ratio = (total[:HEAD_DIM] * (1.0 / norm)).astype(BF16)
            level = top + jnp.log(norm)
            for half in range(2):
                lanes = slice(half * tokens, (half + 1) * tokens)
                b = 2 * t + half
                part[s, b, head * HEAD_DIM : (head + 1) * HEAD_DIM] = ratio[:, lanes]
                lse[s, b, head : head + 1] = level[:, lanes]

        for i in range(len(mine) + 2):
            if i < len(mine):
                score(i)
            if 0 <= i - 1 < len(mine):
                weigh(i - 1)
            if 0 <= i - 2 < len(mine):
                apply(i - 2)

    upper, lower = pl.ds(0, chans // 2), pl.ds(chans // 2, chans // 2)
    hops, plain, merged = [], [], []
    for s in range(samples):

        def to(i, src, dst, target):
            return remote(src, dst, osend.at[s, i], orecv.at[s, i], target)

        hops.append(
            (
                (to(0, part.at[s, 3, upper], hop.at[s, 0], y_next), to(2, lse.at[s, 3], lse_hop.at[s, 0], y_next)),
                (to(1, part.at[s, 3, lower], hop.at[s, 1], y_prev), to(3, lse.at[s, 3], lse_hop.at[s, 1], y_prev)),
            )
        )
        plain.append(
            (
                to(4, part.at[s, 1, upper], part_in.at[s, 1, upper], y_prev),
                to(5, part.at[s, 2, lower], part_in.at[s, 0, lower], y_next),
            )
        )
        merged.append(
            (
                (to(6, part.at[s, 2, upper], part_in.at[s, 0, upper], y_next), to(8, lse.at[s, 2], lse_in.at[s, 0], y_next)),
                (to(7, part.at[s, 1, lower], part_in.at[s, 1, lower], y_prev), to(9, lse.at[s, 1], lse_in.at[s, 1], y_prev)),
            )
        )

    def send_parts(s, n):
        if n < 2:
            hops[s][n][0].start()
        if n == 1:
            hops[s][0][1].start()
            hops[s][1][1].start()
            plain[s][1].start()
        if n == 2:
            plain[s][0].start()

    def relay_parts(s):
        for n, b in ((0, 2), (1, 1)):
            with jax.named_scope("wait_hops"):
                for copy in hops[s][n]:
                    copy.wait_recv()
            with jax.named_scope("add_hops"):
                near_level, far_level = lse[s, b], lse_hop[s, n]
                top = jnp.maximum(near_level, far_level)
                near_scale, far_scale = jnp.exp(near_level - top), jnp.exp(far_level - top)
                total = near_scale + far_scale
                near_scale, far_scale = near_scale / total, far_scale / total
                first = n * heads // 2
                for h in range(first, first + heads // 2):
                    rows = slice(h * HEAD_DIM, (h + 1) * HEAD_DIM)
                    there = slice((h - first) * HEAD_DIM, (h - first + 1) * HEAD_DIM)
                    value = near_scale[h : h + 1] * part[s, b, rows].astype(F32)
                    value = value + far_scale[h : h + 1] * hop[s, n, there].astype(F32)
                    part[s, b, rows] = value.astype(BF16)
                lse[s, b, first : first + heads // 2] = (top + jnp.log(total))[first : first + heads // 2]
            for copy in merged[s][n]:
                copy.start()

    def near_queries(s):
        with jax.named_scope("wait_q_near"):
            qc[s][0].wait_recv()
            qc[s][2].start()
            qc[s][1].wait_recv()
            qc[s][3].start()

    def near_keys(s):
        with jax.named_scope("wait_z_near"):
            zc[s][0].wait_recv()
            zc[s][2].start()
            zc[s][1].wait_recv()
            zc[s][3].start()
        with jax.named_scope("near_pairs"):
            project(zbuf[s, 1:3].reshape(2 * tokens, chans), s, 1, 2)

    def far(s):
        with jax.named_scope("wait_z_far"):
            zc[s][2].wait_recv()
            zc[s][3].wait_recv()
        with jax.named_scope("far_pairs"):
            project(zbuf[s, 3], s, 4, 1)
        first, second = range(heads // 2), range(heads // 2, heads)
        for n, mine in enumerate(([(h, 1) for h in first], [(h, 1) for h in second], [(h, 0) for h in range(heads)])):
            with jax.named_scope("attend_far"):
                attend_far(s, mine)
            send_parts(s, n)

    def wait_far_queries(s):
        with jax.named_scope("wait_q_far"):
            qc[s][2].wait_recv()
            qc[s][3].wait_recv()

    last, gone = SIDE - 1, n_patch - 1
    sends_across = (jnp.logical_and(z == last, y < last), jnp.logical_and(z == 0, y > 0))
    gets_across = jnp.logical_or(jnp.logical_and(z == last, y > 0), jnp.logical_and(z == 0, y < last))
    sends_down = (z < last, jnp.logical_and(z == last, y > 0))
    sends_up = (z > 0, jnp.logical_and(z == 0, y < last))
    across, down, up = [], [], []
    for s in range(samples):

        def rim(i, src, dst, target):
            return remote(src.at[s], dst.at[s], rsend.at[s, i], rrecv.at[s, i], target)

        across.append([rim(2, rim_own, rim_hop, target) for target in (y_next, y_prev)])
        down.append([rim(0, src, rim_near.at[0], z_next) for src in (rim_own, rim_hop)])
        up.append([rim(1, src, rim_near.at[1], z_prev) for src in (rim_own, rim_hop)])

    def start_rims_across():
        loads[5].wait()
        for s in range(samples):
            for condition, copy in zip(sends_across, across[s]):
                pl.when(condition)(copy.start)

    def start_rims(s):
        pl.when(gets_across)(across[s][0].wait_recv)
        for conditions, copies in ((sends_down, down[s]), (sends_up, up[s])):
            for condition, copy in zip(conditions, copies):
                pl.when(condition)(copy.start)

        @pl.when(p == 0)
        def _():
            rim_near[0, s] = jnp.zeros(rim_near.shape[2:], BF16)

        @pl.when(p == gone)
        def _():
            rim_near[1, s] = jnp.zeros(rim_near.shape[2:], BF16)

    near_queries(0)
    near_keys(0)
    near_queries(1)
    start_rims_across()
    wait_far_queries(0)
    with jax.named_scope("attend_near"):
        attend_near(0, units)
    near_keys(1)
    far(0)
    start_rims(0)
    wait_far_queries(1)
    with jax.named_scope("attend_near"):
        attend_near(1, units)
    relay_parts(0)
    far(1)

    with jax.named_scope("wait_loads"):
        for load in loads[6:]:
            load.wait()

    row = lax.broadcasted_iota(jnp.int32, (tokens, chans), 0)

    def merge_columns(left, mid, right):
        lefts = jnp.where(row == 0, 0.0, pltpu.roll(left, 1, 0))
        rights = jnp.where(row == tokens - 1, 0.0, pltpu.roll(right, tokens - 1, 0))
        return lefts + mid + rights

    def far_first(k):
        dy, dz = divmod(k, SIDE)
        return -min(dy, SIDE - dy) - 2 * min(dz, SIDE - dz)

    def finish(s):
        with jax.named_scope("wait_parts"):
            for copy in plain[s] + merged[s][0] + merged[s][1]:
                copy.wait_recv()
        with jax.named_scope("merge"):
            levels = [lse[s, 0], lse_in[s, 0], lse_in[s, 1]]
            top = functools.reduce(jnp.maximum, levels)
            scaled = [jnp.exp(level - top) for level in levels]
            inverse = 1.0 / functools.reduce(jnp.add, scaled)
            shares = [e * inverse for e in scaled]
            for j in range(pairs):
                totals = []
                for h in (2 * j, 2 * j + 1):
                    rows = slice(h * HEAD_DIM, (h + 1) * HEAD_DIM)
                    total = shares[0][h : h + 1] * part[s, 0, rows].astype(F32)
                    for b in range(2):
                        total = total + shares[b + 1][h : h + 1] * part_in[s, b, rows].astype(F32)
                    totals.append(total)
                att[s, :, j * 128 : (j + 1) * 128] = jnp.concatenate(totals, 0).T.astype(BF16)
        with jax.named_scope("out_proj"):
            for cols in blocks:
                value = hidden[s, :, cols].astype(F32) + dot(att[s], w_out[:, cols])
                value = value.astype(BF16)
                res[s, :, cols] = value
                value = value.astype(F32)
                mean = jnp.mean(value, 0, keepdims=True)
                centred = value - mean
                gst[s, 0, 0:1, cols] = mean
                gst[s, 0, 1:2, cols] = jnp.sum(centred * centred, 0, keepdims=True)
        copies = [
            remote(gst.at[s, 0], gst.at[s, k], gsend.at[s, k - 1], grecv.at[s, k - 1], peer(k))
            for k in range(1, n_patch)
        ]
        for k in sorted(range(1, n_patch), key=far_first):
            copies[k - 1].start()
        return copies

    def group_sum(values):
        high = values.astype(BF16).astype(F32)
        rest = values - high
        mid = rest.astype(BF16).astype(F32)
        tail = rest - mid
        stack = jnp.concatenate([high, mid, tail, jnp.zeros((5, chans), F32)], 0).astype(BF16)
        sums = dot(stack, proj[...])
        return sums[0:1] + sums[1:2] + sums[2:3]

    def normalise(s, copies):
        with jax.named_scope("wait_stats"):
            for copy in copies:
                copy.wait_recv()
        with jax.named_scope("stats"):
            stats = [gst[s, k] for k in range(n_patch)]
            mean = group_sum(functools.reduce(jnp.add, stats)[0:1] / n_patch) / width
            squares = jnp.zeros((1, chans), F32)
            for stat in stats:
                gap = stat[0:1] - mean
                squares = squares + (stat[1:2] + tokens * (gap * gap))
            var = group_sum(squares) / (n_patch * tokens * width)
            rate = lax.rsqrt(var + EPSILON)
        with jax.named_scope("silu"):
            for r in range(0, tokens, 32):
                value = (res[s, r : r + 32].astype(F32) - mean) * rate
                value = value * gn_gain[...].reshape(1, chans) + gn_bias[...].reshape(1, chans)
                act[s, r : r + 32] = (value / (1.0 + jnp.exp(-value))).astype(BF16)
        with jax.named_scope("conv"):
            taps = [dot(act[s], conv_w[1, b]) for b in range(3)]
            out[s] = (merge_columns(*taps) + rim_sum[s] + res[s].astype(F32)).astype(BF16)

    def rim_taps(s):
        with jax.named_scope("wait_rims"):
            pl.when(p > 0)(down[s][0].wait_recv)
            pl.when(p < gone)(up[s][0].wait_recv)
        with jax.named_scope("rim_taps"):
            taps = [dot(rim_near[0, s], conv_w[0, b]) + dot(rim_near[1, s], conv_w[2, b]) for b in range(3)]
            rim_sum[s] = merge_columns(*taps) + conv_b[...].reshape(1, chans) + shift[s : s + 1]

    stat_copies = [finish(0)]
    start_rims(1)
    relay_parts(1)
    stat_copies.append(finish(1))
    rim_taps(0)
    normalise(0, stat_copies[0])
    rim_taps(1)
    normalise(1, stat_copies[1])

    for s in range(samples):
        for copy in zc[s] + qc[s]:
            copy.wait_send()
        for copy in hops[s][0] + hops[s][1] + plain[s] + merged[s][0] + merged[s][1] + tuple(stat_copies[s]):
            copy.wait_send()
        for conditions, copies in ((sends_across, across[s]), (sends_down, down[s]), (sends_up, up[s])):
            for condition, copy in zip(conditions, copies):
                pl.when(condition)(copy.wait_send)


def shards(
    hidden,
    stale_attn_in,
    stale_conv_in,
    ln_gain,
    ln_bias,
    w_qkv,
    w_out,
    gn_gain,
    gn_bias,
    conv_weight,
    conv_bias,
    time_shift,
):
    samples, rows, tokens, chans = hidden.shape
    block = (samples, rows * tokens, chans)
    operands = (
        hidden.reshape(block),
        stale_attn_in.reshape(block),
        stale_conv_in.reshape(block),
        ln_gain,
        ln_bias,
        w_qkv,
        w_out,
        gn_gain,
        gn_bias,
        conv_weight,
        conv_bias,
        time_shift,
    )
    dma = pltpu.SemaphoreType.DMA
    vector = pltpu.VMEM((chans,), F32)
    out = pl.pallas_call(
        kernel,
        out_shape=jax.ShapeDtypeStruct(block, BF16),
        in_specs=[pl.BlockSpec(memory_space=pl.ANY)] * len(operands),
        out_specs=pl.BlockSpec(memory_space=pltpu.VMEM),
        scratch_shapes=[
            pltpu.VMEM(block, BF16),
            pltpu.VMEM(block, BF16),
            pltpu.VMEM(block, BF16),
            pltpu.VMEM((2,) + block, BF16),
            pltpu.VMEM(block, BF16),
            vector,
            vector,
            pltpu.VMEM(w_qkv.shape, BF16),
            pltpu.VMEM(w_out.shape, BF16),
            vector,
            vector,
            pltpu.VMEM(conv_weight.shape, BF16),
            vector,
            pltpu.VMEM(time_shift.shape, F32),
            pltpu.VMEM(block, BF16),
            pltpu.VMEM((samples, SIDE, tokens, chans), BF16),
            pltpu.VMEM((samples, SIDE, tokens, chans), BF16),
            pltpu.VMEM((samples, 5 * tokens, chans), BF16),
            pltpu.VMEM((chans, chans), BF16),
            pltpu.VMEM((samples, chans // HEAD_DIM * HEAD_ROWS, 5 * tokens), BF16),
            pltpu.VMEM((4, 4 * tokens, 2 * tokens), F32),
            pltpu.VMEM((4, 4 * tokens, 2 * tokens), BF16),
            pltpu.VMEM((samples, 2, chans // HEAD_DIM * HEAD_ROWS, 2 * tokens), F32),
            pltpu.VMEM((samples, SIDE, chans, tokens), BF16),
            pltpu.VMEM((samples, 2, chans, tokens), BF16),
            pltpu.VMEM((samples, 2, chans // 2, tokens), BF16),
            pltpu.VMEM((samples, SIDE, 16, tokens), F32),
            pltpu.VMEM((samples, 2, 16, tokens), F32),
            pltpu.VMEM((samples, 2, 16, tokens), F32),
            pltpu.VMEM(block, BF16),
            pltpu.VMEM(block, BF16),
            pltpu.VMEM((samples, SIDE * SIDE, 2, chans), F32),
            pltpu.VMEM((chans, chans), BF16),
            pltpu.VMEM(block, F32),
            pltpu.VMEM(block, BF16),
            dma((12,)),
            dma((samples, 4)),
            dma((samples, 4)),
            dma((samples, 4)),
            dma((samples, 4)),
            dma((samples, 10)),
            dma((samples, 10)),
            dma((samples, 3)),
            dma((samples, 3)),
            dma((samples, SIDE * SIDE - 1)),
            dma((samples, SIDE * SIDE - 1)),
        ],
        compiler_params=pltpu.CompilerParams(
            collective_id=0, has_side_effects=True, vmem_limit_bytes=42 * 1024 * 1024
        ),
        name="section",
    )(*[pltpu.with_memory_space_constraint(x, pltpu.HBM) for x in operands])
    return out.reshape(hidden.shape)


def solution(mesh):
    spread = P("img", "patch", None, None)
    return jax.shard_map(
        shards,
        mesh=mesh,
        in_specs=(spread, spread, spread) + (P(),) * 8 + (P("img", None),),
        out_specs=spread,
        check_vma=False,
    )
```

```python
import functools

import jax
import jax.numpy as jnp
from jax import lax
from jax.experimental import pallas as pl
from jax.experimental.pallas import tpu as pltpu
from jax.sharding import PartitionSpec as P

GROUPS = 32
HEAD_DIM = 64
HEAD_ROWS = 80
SIDE = 4
EPSILON = 1e-05
MESH = pl.DeviceIdType.MESH
F32 = jnp.float32
BF16 = jnp.bfloat16


def dot_nt(a, b):
    return lax.dot_general(a, b, (((1,), (1,)), ((), ())), preferred_element_type=F32)


def dot(a, b):
    return jnp.dot(a, b, preferred_element_type=F32)


def kernel(
    hidden_hbm,
    stale_hbm,
    rim_hbm,
    ln_gain_hbm,
    ln_bias_hbm,
    w_qkv_hbm,
    w_out_hbm,
    gn_gain_hbm,
    gn_bias_hbm,
    conv_w_hbm,
    conv_b_hbm,
    shift_hbm,
    out,
    hidden,
    stale,
    rim_own,
    rim_near,
    rim_hop,
    ln_gain,
    ln_bias,
    w_qkv,
    w_out,
    gn_gain,
    gn_bias,
    conv_w,
    conv_b,
    shift,
    fresh,
    zbuf,
    qbuf,
    kbuf,
    w_vt,
    vt,
    scores,
    weights,
    sums,
    part,
    part_in,
    hop,
    lse,
    lse_in,
    lse_hop,
    att,
    res,
    gst,
    proj,
    rim_sum,
    act,
    load_sem,
    zsend,
    zrecv,
    qsend,
    qrecv,
    osend,
    orecv,
    rsend,
    rrecv,
    gsend,
    grecv,
):
    n_patch = SIDE * SIDE
    samples, tokens, chans = hidden.shape
    half = tokens // 2
    p = lax.axis_index("patch")
    y, z = p // SIDE, p % SIDE
    z_next = {"patch": y * SIDE + (z + 1) % SIDE}
    z_prev = {"patch": y * SIDE + (z + SIDE - 1) % SIDE}
    y_next = {"patch": ((y + 1) % SIDE) * SIDE + z}
    y_prev = {"patch": ((y + SIDE - 1) % SIDE) * SIDE + z}

    def peer(k):
        return {"patch": (p + k) % n_patch}

    loads = []
    for i, (src, dst) in enumerate(
        (
            (stale_hbm, stale),
            (ln_gain_hbm, ln_gain),
            (ln_bias_hbm, ln_bias),
            (hidden_hbm, hidden),
            (w_qkv_hbm, w_qkv),
            (rim_hbm, rim_own),
            (w_out_hbm, w_out),
            (gn_gain_hbm, gn_gain),
            (gn_bias_hbm, gn_bias),
            (conv_b_hbm, conv_b),
            (shift_hbm, shift),
            (conv_w_hbm, conv_w),
        )
    ):
        load = pltpu.make_async_copy(src, dst, load_sem.at[i])
        load.start()
        loads.append(load)

    barrier = pltpu.get_barrier_semaphore()
    for target in (z_next, z_prev, y_next, y_prev):
        pl.semaphore_signal(barrier, inc=1, device_id=target, device_id_type=MESH)

    def remote(src, dst, send, recv, target):
        return pltpu.make_async_remote_copy(
            src_ref=src, dst_ref=dst, send_sem=send, recv_sem=recv, device_id=target, device_id_type=MESH
        )

    def ring(buf, send, recv, s, nxt, prv):
        return (
            remote(buf.at[s, 0], buf.at[s, 1], send.at[s, 0], recv.at[s, 0], nxt),
            remote(buf.at[s, 0], buf.at[s, 2], send.at[s, 1], recv.at[s, 1], prv),
            remote(
                buf.at[s, 1, pl.ds(0, half)], buf.at[s, 3, pl.ds(0, half)], send.at[s, 2], recv.at[s, 2], nxt
            ),
            remote(
                buf.at[s, 2, pl.ds(half, half)],
                buf.at[s, 3, pl.ds(half, half)],
                send.at[s, 3],
                recv.at[s, 3],
                prv,
            ),
        )

    zc = [ring(zbuf, zsend, zrecv, s, z_next, z_prev) for s in range(samples)]
    qc = [ring(qbuf, qsend, qrecv, s, y_next, y_prev) for s in range(samples)]

    def layer_norm(values):
        values = values.astype(F32)
        centre = jnp.mean(values, -1, keepdims=True)
        centred = values - centre
        spread = jnp.mean(centred * centred, -1, keepdims=True)
        return (centred * lax.rsqrt(spread + EPSILON) * ln_gain[...].reshape(1, chans) + ln_bias[...].reshape(1, chans)).astype(BF16)

    step = 32
    blocks = [slice(c, min(c + 256, chans)) for c in range(0, chans, 256)]
    def norm_stale(s):
        with jax.named_scope("norm_stale"):

            @pl.loop(0, tokens // step, unroll=True)
            def _(i):
                rows = pl.ds(pl.multiple_of(i * step, step), step)
                zbuf[s, 0, rows] = layer_norm(stale[s, rows])

    for load in loads[:3]:
        load.wait()
    norm_stale(0)
    with jax.named_scope("barrier"):
        pl.semaphore_wait(barrier, 4)
    for s in range(samples):
        if s > 0:
            norm_stale(s)
        zc[s][0].start()
        zc[s][1].start()

    with jax.named_scope("norm_fresh"):
        loads[3].wait()
        for s in range(samples):

            @pl.loop(0, tokens // step, unroll=True)
            def _(i):
                rows = pl.ds(pl.multiple_of(i * step, step), step)
                fresh[s, rows] = layer_norm(hidden[s, rows])

    with jax.named_scope("turn_weights"):
        lse[...] = jnp.zeros(lse.shape, F32)
        loads[4].wait()
        for r in range(0, chans, 128):
            for c in range(0, chans, 128):
                block = w_qkv[r : r + 128, 2 * chans + c : 2 * chans + c + 128]
                w_vt[c : c + 128, r : r + 128] = block.astype(F32).T.astype(BF16)
        for u in range(2):
            weights[2 * u, 3 * tokens :, :tokens] = jnp.zeros((tokens, tokens), BF16)
            weights[2 * u, :tokens, tokens:] = jnp.zeros((tokens, tokens), BF16)

    with jax.named_scope("queries"):
        for s in range(samples):
            for cols in blocks:
                q = dot(fresh[s], w_qkv[:, cols]).astype(BF16)
                qbuf[s, 0, :, cols] = q * BF16(HEAD_DIM**-0.5)
            qc[s][0].start()
            qc[s][1].start()

    heads = chans // HEAD_DIM

    def project(src, s, block, count):
        rows = slice(block * tokens, (block + count) * tokens)
        for cols in blocks:
            kbuf[s, rows, cols] = dot(src, w_qkv[:, chans + cols.start : chans + cols.stop]).astype(BF16)
        values = dot_nt(w_vt[...], src).astype(BF16)
        for h in range(heads):
            vt[s, h * HEAD_ROWS : h * HEAD_ROWS + HEAD_DIM, rows] = values[h * HEAD_DIM : (h + 1) * HEAD_DIM]

    with jax.named_scope("own_pairs"):
        for s in range(samples):
            project(fresh[s], s, 0, 1)
            project(zbuf[s, 0], s, 3, 1)
            for h in range(heads):
                vt[s, h * HEAD_ROWS + HEAD_DIM : (h + 1) * HEAD_ROWS, :] = jnp.ones(
                    (HEAD_ROWS - HEAD_DIM, 5 * tokens), BF16
                )

    width = chans // GROUPS

    def group_of(v):
        return (v * (65536 // width + 1)) >> 16

    for r in range(0, chans, 128):
        same = group_of(lax.broadcasted_iota(jnp.int32, (128, chans), 0) + r) == group_of(
            lax.broadcasted_iota(jnp.int32, (128, chans), 1)
        )
        proj[r : r + 128] = jnp.where(same, 1.0, 0.0).astype(BF16)

    keys = 3 * tokens
    pairs = chans // 128
    low = lax.broadcasted_iota(jnp.int32, (2 * tokens, 128), 1) < HEAD_DIM
    units = [(head, t) for head in range(heads) for t in range(2)]

    def masked_queries(s, head, t):
        cols = slice(head // 2 * 128, head // 2 * 128 + 128)
        queries = qbuf[s, 2 * t : 2 * t + 2, :, cols].reshape(2 * tokens, 128)
        return cols, jnp.where(low if head % 2 == 0 else ~low, queries, BF16(0))

    def attend_near(s, units):
        peaks = {}

        def score(i):
            head, t = units[i]
            u = i % 4
            first = 0 if t == 0 else tokens
            cols, queries = masked_queries(s, head, t)
            value = dot_nt(kbuf[s, first : 4 * tokens, cols], queries)
            if t == 0:
                scores[u] = value
                peaks[i] = (
                    jnp.max(value[:keys, :tokens], 0, keepdims=True),
                    jnp.max(value[tokens:, tokens:], 0, keepdims=True),
                )
            else:
                scores[u, tokens:] = value
                top = jnp.max(value, 0, keepdims=True)
                peaks[i] = (top[:, :tokens], top[:, tokens:])

        def apply(i):
            head, t = units[i]
            u = i % 4
            for half, top in enumerate(peaks[i]):
                lanes = slice(half * tokens, (half + 1) * tokens)
                first = 0 if t == 0 and half == 0 else tokens
                rows = slice(first, first + keys)
                weights[u, rows, lanes] = jnp.exp(scores[u, rows, lanes] - top).astype(BF16)
            mine = slice(head * HEAD_ROWS, (head + 1) * HEAD_ROWS)
            first = 0 if t == 0 else tokens
            sums[s, t, mine] = dot(vt[s, mine, first : 4 * tokens], weights[u, first:])
            spare = slice(head * HEAD_ROWS + HEAD_DIM + 8, (head + 1) * HEAD_ROWS)
            sums[s, t, spare] = jnp.broadcast_to(jnp.concatenate(peaks[i], 1), (8, 2 * tokens))

        ahead = 3
        for i in range(len(units) + ahead):
            if i < len(units):
                score(i)
            if i >= ahead:
                apply(i - ahead)

    def attend_far(s, mine):
        values, gains = {}, {}

        def score(i):
            head, t = mine[i]
            cols, queries = masked_queries(s, head, t)
            values[i] = dot_nt(kbuf[s, 4 * tokens :, cols], queries)

        def weigh(i):
            head, t = mine[i]
            spare = slice(head * HEAD_ROWS + HEAD_DIM + 8, (head + 1) * HEAD_ROWS)
            before = sums[s, t, spare][0:1]
            top = jnp.maximum(before, jnp.max(values[i], 0, keepdims=True))
            gains[i] = (jnp.exp(before - top), top)
            values[i] = jnp.exp(values[i] - top).astype(BF16)

        def apply(i):
            head, t = mine[i]
            gain, top = gains[i]
            rows = slice(head * HEAD_ROWS, (head + 1) * HEAD_ROWS)
            total = sums[s, t, rows] * gain + dot(vt[s, rows, 4 * tokens :], values[i])
            norm = total[HEAD_DIM : HEAD_DIM + 1]
            ratio = (total[:HEAD_DIM] * (1.0 / norm)).astype(BF16)
            level = top + jnp.log(norm)
            for half in range(2):
                lanes = slice(half * tokens, (half + 1) * tokens)
                b = 2 * t + half
                part[s, b, head * HEAD_DIM : (head + 1) * HEAD_DIM] = ratio[:, lanes]
                lse[s, b, head : head + 1] = level[:, lanes]

        for i in range(len(mine) + 2):
            if i < len(mine):
                score(i)
            if 0 <= i - 1 < len(mine):
                weigh(i - 1)
            if 0 <= i - 2 < len(mine):
                apply(i - 2)

    upper, lower = pl.ds(0, chans // 2), pl.ds(chans // 2, chans // 2)
    hops, plain, merged = [], [], []
    for s in range(samples):

        def to(i, src, dst, target):
            return remote(src, dst, osend.at[s, i], orecv.at[s, i], target)

        hops.append(
            (
                (to(0, part.at[s, 3, upper], hop.at[s, 0], y_next), to(2, lse.at[s, 3], lse_hop.at[s, 0], y_next)),
                (to(1, part.at[s, 3, lower], hop.at[s, 1], y_prev), to(3, lse.at[s, 3], lse_hop.at[s, 1], y_prev)),
            )
        )
        plain.append(
            (
                to(4, part.at[s, 1, upper], part_in.at[s, 1, upper], y_prev),
                to(5, part.at[s, 2, lower], part_in.at[s, 0, lower], y_next),
            )
        )
        merged.append(
            (
                (to(6, part.at[s, 2, upper], part_in.at[s, 0, upper], y_next), to(8, lse.at[s, 2], lse_in.at[s, 0], y_next)),
                (to(7, part.at[s, 1, lower], part_in.at[s, 1, lower], y_prev), to(9, lse.at[s, 1], lse_in.at[s, 1], y_prev)),
            )
        )

    def send_parts(s, n):
        if n < 2:
            hops[s][n][0].start()
        if n == 1:
            hops[s][0][1].start()
            hops[s][1][1].start()
            plain[s][1].start()
        if n == 2:
            plain[s][0].start()

    def relay_parts(s):
        for n, b in ((0, 2), (1, 1)):
            with jax.named_scope("wait_hops"):
                for copy in hops[s][n]:
                    copy.wait_recv()
            with jax.named_scope("add_hops"):
                near_level, far_level = lse[s, b], lse_hop[s, n]
                top = jnp.maximum(near_level, far_level)
                near_scale, far_scale = jnp.exp(near_level - top), jnp.exp(far_level - top)
                total = near_scale + far_scale
                near_scale, far_scale = near_scale / total, far_scale / total
                first = n * heads // 2
                for h in range(first, first + heads // 2):
                    rows = slice(h * HEAD_DIM, (h + 1) * HEAD_DIM)
                    there = slice((h - first) * HEAD_DIM, (h - first + 1) * HEAD_DIM)
                    value = near_scale[h : h + 1] * part[s, b, rows].astype(F32)
                    value = value + far_scale[h : h + 1] * hop[s, n, there].astype(F32)
                    part[s, b, rows] = value.astype(BF16)
                lse[s, b, first : first + heads // 2] = (top + jnp.log(total))[first : first + heads // 2]
            for copy in merged[s][n]:
                copy.start()

    def near_queries(s):
        with jax.named_scope("wait_q_near"):
            qc[s][0].wait_recv()
            qc[s][2].start()
            qc[s][1].wait_recv()
            qc[s][3].start()

    def near_keys(s):
        with jax.named_scope("wait_z_near"):
            zc[s][0].wait_recv()
            zc[s][2].start()
            zc[s][1].wait_recv()
            zc[s][3].start()
        with jax.named_scope("near_pairs"):
            project(zbuf[s, 1:3].reshape(2 * tokens, chans), s, 1, 2)

    def far(s):
        with jax.named_scope("wait_z_far"):
            zc[s][2].wait_recv()
            zc[s][3].wait_recv()
        with jax.named_scope("far_pairs"):
            project(zbuf[s, 3], s, 4, 1)
        first, second = range(heads // 2), range(heads // 2, heads)
        for n, mine in enumerate(([(h, 1) for h in first], [(h, 1) for h in second], [(h, 0) for h in range(heads)])):
            with jax.named_scope("attend_far"):
                attend_far(s, mine)
            send_parts(s, n)
            if s == 0 and n == 0:
                start_rims(0)

    def wait_far_queries(s):
        with jax.named_scope("wait_q_far"):
            qc[s][2].wait_recv()
            qc[s][3].wait_recv()

    last, gone = SIDE - 1, n_patch - 1
    sends_across = (jnp.logical_and(z == last, y < last), jnp.logical_and(z == 0, y > 0))
    gets_across = jnp.logical_or(jnp.logical_and(z == last, y > 0), jnp.logical_and(z == 0, y < last))
    sends_down = (z < last, jnp.logical_and(z == last, y > 0))
    sends_up = (z > 0, jnp.logical_and(z == 0, y < last))
    across, down, up = [], [], []
    for s in range(samples):

        def rim(i, src, dst, target):
            return remote(src.at[s], dst.at[s], rsend.at[s, i], rrecv.at[s, i], target)

        across.append([rim(2, rim_own, rim_hop, target) for target in (y_next, y_prev)])
        down.append([rim(0, src, rim_near.at[0], z_next) for src in (rim_own, rim_hop)])
        up.append([rim(1, src, rim_near.at[1], z_prev) for src in (rim_own, rim_hop)])

    def start_rims_across():
        loads[5].wait()
        for s in range(samples):
            for condition, copy in zip(sends_across, across[s]):
                pl.when(condition)(copy.start)

    def start_rims(s):
        pl.when(gets_across)(across[s][0].wait_recv)
        for conditions, copies in ((sends_down, down[s]), (sends_up, up[s])):
            for condition, copy in zip(conditions, copies):
                pl.when(condition)(copy.start)

        @pl.when(p == 0)
        def _():
            rim_near[0, s] = jnp.zeros(rim_near.shape[2:], BF16)

        @pl.when(p == gone)
        def _():
            rim_near[1, s] = jnp.zeros(rim_near.shape[2:], BF16)

    near_queries(0)
    near_keys(0)
    near_queries(1)
    start_rims_across()
    wait_far_queries(0)
    with jax.named_scope("attend_near"):
        attend_near(0, units)
    near_keys(1)
    far(0)
    wait_far_queries(1)
    with jax.named_scope("attend_near"):
        attend_near(1, units)
    relay_parts(0)
    far(1)
    start_rims(1)

    with jax.named_scope("wait_loads"):
        for load in loads[6:]:
            load.wait()

    row = lax.broadcasted_iota(jnp.int32, (tokens, chans), 0)

    def merge_columns(left, mid, right):
        lefts = jnp.where(row == 0, 0.0, pltpu.roll(left, 1, 0))
        rights = jnp.where(row == tokens - 1, 0.0, pltpu.roll(right, tokens - 1, 0))
        return lefts + mid + rights

    def far_first(k):
        dy, dz = divmod(k, SIDE)
        return -min(dy, SIDE - dy) - 2 * min(dz, SIDE - dz)

    def finish(s):
        with jax.named_scope("wait_parts"):
            for copy in plain[s] + merged[s][0] + merged[s][1]:
                copy.wait_recv()
        with jax.named_scope("merge"):
            levels = [lse[s, 0], lse_in[s, 0], lse_in[s, 1]]
            top = functools.reduce(jnp.maximum, levels)
            scaled = [jnp.exp(level - top) for level in levels]
            inverse = 1.0 / functools.reduce(jnp.add, scaled)
            shares = [e * inverse for e in scaled]
            for j in range(pairs):
                totals = []
                for h in (2 * j, 2 * j + 1):
                    rows = slice(h * HEAD_DIM, (h + 1) * HEAD_DIM)
                    total = shares[0][h : h + 1] * part[s, 0, rows].astype(F32)
                    for b in range(2):
                        total = total + shares[b + 1][h : h + 1] * part_in[s, b, rows].astype(F32)
                    totals.append(total)
                att[s, :, j * 128 : (j + 1) * 128] = jnp.concatenate(totals, 0).T.astype(BF16)
        with jax.named_scope("out_proj"):
            for cols in blocks:
                value = hidden[s, :, cols].astype(F32) + dot(att[s], w_out[:, cols])
                value = value.astype(BF16)
                res[s, :, cols] = value
                value = value.astype(F32)
                mean = jnp.mean(value, 0, keepdims=True)
                centred = value - mean
                gst[s, 0, 0:1, cols] = mean
                gst[s, 0, 1:2, cols] = jnp.sum(centred * centred, 0, keepdims=True)
        copies = [
            remote(gst.at[s, 0], gst.at[s, k], gsend.at[s, k - 1], grecv.at[s, k - 1], peer(k))
            for k in range(1, n_patch)
        ]
        for k in sorted(range(1, n_patch), key=far_first):
            copies[k - 1].start()
        return copies

    def group_sum(values):
        high = values.astype(BF16).astype(F32)
        rest = values - high
        mid = rest.astype(BF16).astype(F32)
        tail = rest - mid
        stack = jnp.concatenate([high, mid, tail, jnp.zeros((5, chans), F32)], 0).astype(BF16)
        sums = dot(stack, proj[...])
        return sums[0:1] + sums[1:2] + sums[2:3]

    def normalise(s, copies):
        with jax.named_scope("wait_stats"):
            for copy in copies:
                copy.wait_recv()
        with jax.named_scope("stats"):
            stats = [gst[s, k] for k in range(n_patch)]
            mean = group_sum(functools.reduce(jnp.add, stats)[0:1] / n_patch) / width
            squares = jnp.zeros((1, chans), F32)
            for stat in stats:
                gap = stat[0:1] - mean
                squares = squares + (stat[1:2] + tokens * (gap * gap))
            var = group_sum(squares) / (n_patch * tokens * width)
            rate = lax.rsqrt(var + EPSILON)
        with jax.named_scope("silu"):
            for r in range(0, tokens, 32):
                value = (res[s, r : r + 32].astype(F32) - mean) * rate
                value = value * gn_gain[...].reshape(1, chans) + gn_bias[...].reshape(1, chans)
                act[s, r : r + 32] = (value / (1.0 + jnp.exp(-value))).astype(BF16)
        with jax.named_scope("conv"):
            taps = [dot(act[s], conv_w[1, b]) for b in range(3)]
            out[s] = (merge_columns(*taps) + rim_sum[s] + res[s].astype(F32)).astype(BF16)

    def rim_taps(s):
        with jax.named_scope("wait_rims"):
            pl.when(p > 0)(down[s][0].wait_recv)
            pl.when(p < gone)(up[s][0].wait_recv)
        with jax.named_scope("rim_taps"):
            taps = [dot(rim_near[0, s], conv_w[0, b]) + dot(rim_near[1, s], conv_w[2, b]) for b in range(3)]
            rim_sum[s] = merge_columns(*taps) + conv_b[...].reshape(1, chans) + shift[s : s + 1]

    stat_copies = [finish(0)]
    relay_parts(1)
    stat_copies.append(finish(1))
    rim_taps(0)
    normalise(0, stat_copies[0])
    rim_taps(1)
    normalise(1, stat_copies[1])

    for s in range(samples):
        for copy in zc[s] + qc[s]:
            copy.wait_send()
        for copy in hops[s][0] + hops[s][1] + plain[s] + merged[s][0] + merged[s][1] + tuple(stat_copies[s]):
            copy.wait_send()
        for conditions, copies in ((sends_across, across[s]), (sends_down, down[s]), (sends_up, up[s])):
            for condition, copy in zip(conditions, copies):
                pl.when(condition)(copy.wait_send)


def shards(
    hidden,
    stale_attn_in,
    stale_conv_in,
    ln_gain,
    ln_bias,
    w_qkv,
    w_out,
    gn_gain,
    gn_bias,
    conv_weight,
    conv_bias,
    time_shift,
):
    samples, rows, tokens, chans = hidden.shape
    block = (samples, rows * tokens, chans)
    operands = (
        hidden.reshape(block),
        stale_attn_in.reshape(block),
        stale_conv_in.reshape(block),
        ln_gain,
        ln_bias,
        w_qkv,
        w_out,
        gn_gain,
        gn_bias,
        conv_weight,
        conv_bias,
        time_shift,
    )
    dma = pltpu.SemaphoreType.DMA
    vector = pltpu.VMEM((chans,), F32)
    out = pl.pallas_call(
        kernel,
        out_shape=jax.ShapeDtypeStruct(block, BF16),
        in_specs=[pl.BlockSpec(memory_space=pl.ANY)] * len(operands),
        out_specs=pl.BlockSpec(memory_space=pltpu.VMEM),
        scratch_shapes=[
            pltpu.VMEM(block, BF16),
            pltpu.VMEM(block, BF16),
            pltpu.VMEM(block, BF16),
            pltpu.VMEM((2,) + block, BF16),
            pltpu.VMEM(block, BF16),
            vector,
            vector,
            pltpu.VMEM(w_qkv.shape, BF16),
            pltpu.VMEM(w_out.shape, BF16),
            vector,
            vector,
            pltpu.VMEM(conv_weight.shape, BF16),
            vector,
            pltpu.VMEM(time_shift.shape, F32),
            pltpu.VMEM(block, BF16),
            pltpu.VMEM((samples, SIDE, tokens, chans), BF16),
            pltpu.VMEM((samples, SIDE, tokens, chans), BF16),
            pltpu.VMEM((samples, 5 * tokens, chans), BF16),
            pltpu.VMEM((chans, chans), BF16),
            pltpu.VMEM((samples, chans // HEAD_DIM * HEAD_ROWS, 5 * tokens), BF16),
            pltpu.VMEM((4, 4 * tokens, 2 * tokens), F32),
            pltpu.VMEM((4, 4 * tokens, 2 * tokens), BF16),
            pltpu.VMEM((samples, 2, chans // HEAD_DIM * HEAD_ROWS, 2 * tokens), F32),
            pltpu.VMEM((samples, SIDE, chans, tokens), BF16),
            pltpu.VMEM((samples, 2, chans, tokens), BF16),
            pltpu.VMEM((samples, 2, chans // 2, tokens), BF16),
            pltpu.VMEM((samples, SIDE, 16, tokens), F32),
            pltpu.VMEM((samples, 2, 16, tokens), F32),
            pltpu.VMEM((samples, 2, 16, tokens), F32),
            pltpu.VMEM(block, BF16),
            pltpu.VMEM(block, BF16),
            pltpu.VMEM((samples, SIDE * SIDE, 2, chans), F32),
            pltpu.VMEM((chans, chans), BF16),
            pltpu.VMEM(block, F32),
            pltpu.VMEM(block, BF16),
            dma((12,)),
            dma((samples, 4)),
            dma((samples, 4)),
            dma((samples, 4)),
            dma((samples, 4)),
            dma((samples, 10)),
            dma((samples, 10)),
            dma((samples, 3)),
            dma((samples, 3)),
            dma((samples, SIDE * SIDE - 1)),
            dma((samples, SIDE * SIDE - 1)),
        ],
        compiler_params=pltpu.CompilerParams(
            collective_id=0, has_side_effects=True, vmem_limit_bytes=42 * 1024 * 1024
        ),
        name="section",
    )(*[pltpu.with_memory_space_constraint(x, pltpu.HBM) for x in operands])
    return out.reshape(hidden.shape)


def solution(mesh):
    spread = P("img", "patch", None, None)
    return jax.shard_map(
        shards,
        mesh=mesh,
        in_specs=(spread, spread, spread) + (P(),) * 8 + (P("img", None),),
        out_specs=spread,
        check_vma=False,
    )
```
